32 devices in a mesh: dp: 4 (over x, y), tp: 8 (over z, core).
Axes of the slice: x: 2, y: 2, z: 4, core: 2. Of those that a mesh axis runs over, the one named last changes fastest.
Arguments:
- x: bfloat16 [8, 512, 4096], P('dp', 'tp'), parts along dimension 0
- k_cache: bfloat16 [8, 4096, 32, 128], P('dp', None, 'tp'), parts along dimension 0
- v_cache: bfloat16 [8, 4096, 32, 128], P('dp', None, 'tp'), parts along dimension 0
- prefix_len: int32 [8], P('dp'), parts along dimension 0
- valid_len: int32 [8], P('dp'), parts along dimension 0
- g_attn: bfloat16 [4096], replicated
- w_q: bfloat16 [4096, 4096], P(None, 'tp')
- b_q: bfloat16 [4096], P('tp')
- w_k: bfloat16 [4096, 4096], P(None, 'tp')
- b_k: bfloat16 [4096], P('tp')
- w_v: bfloat16 [4096, 4096], P(None, 'tp')
- b_v: bfloat16 [4096], P('tp')
- w_o: bfloat16 [4096, 4096], P('tp')
- g_mlp: bfloat16 [4096], replicated
- w_gate: bfloat16 [4096, 11008], P(None, 'tp')
- w_up: bfloat16 [4096, 11008], P(None, 'tp')
- w_down: bfloat16 [11008, 4096], P('tp')
Outputs:
- output 1: bfloat16 [8, 512, 4096], P('dp', 'tp'), parts along dimension 0
- output 2: bfloat16 [8, 4096, 32, 128], P('dp', None, 'tp'), parts along dimension 0
- output 3: bfloat16 [8, 4096, 32, 128], P('dp', None, 'tp'), parts along dimension 0
There are 4 independent parts. The reference program is written for one: setup_inputs(seed, part) draws one part's arguments, and reference() takes and returns one part's arrays. A program takes and returns all parts, laid end to end along the dimension named above; an argument that names none is the same for every part.
All inputs are finite; a program needn't handle non-finite values.
Results may differ from the reference program's by a relative error of at most 0.0176057.
Values are sent between devices in bfloat16 or wider.
A program may use at most 1 GiB of HBM per device.

```python
import jax
import jax.numpy as jnp
from jax import lax

REQUESTS = 2
CHUNK_LEN = 512
CACHE_SLOTS = 4096
MODEL_DIM = 4096
NUM_HEADS = 32
KV_HEADS = 32
KV_STORE = 32
HEAD_DIM = 128
FFN_DIM = 11008

ROPE_THETA = 1.0e6
NORM_EPS = 1.0e-6
GROUP_SIZE = NUM_HEADS // KV_STORE
KV_REPEAT = KV_STORE // KV_HEADS


def draw_lengths(key):
    keys = jax.random.split(key, 4)
    prefix = jax.random.randint(keys[0], (REQUESTS,), 0, CACHE_SLOTS - CHUNK_LEN + 1)
    valid = jax.random.randint(keys[1], (REQUESTS,), 1, CHUNK_LEN + 1)
    req_ids = jnp.arange(REQUESTS)
    longest = jax.random.randint(keys[2], (), 0, REQUESTS)
    fullest = jax.random.randint(keys[3], (), 0, REQUESTS)
    prefix = jnp.where(req_ids == longest, CACHE_SLOTS - CHUNK_LEN, prefix)
    valid = jnp.where(req_ids == fullest, CHUNK_LEN, valid)
    return prefix.astype(jnp.int32), valid.astype(jnp.int32)


def gauss(key, shape, scale):
    return jax.random.normal(key, shape, jnp.float32) * scale


def kv_copies(values, axis):
    return jnp.repeat(values, KV_REPEAT, axis=axis)


def setup_inputs(seed: int = 0, part: int = 0) -> dict:
    shared = jax.random.split(jax.random.key(seed), 12)
    local = jax.random.split(jax.random.fold_in(jax.random.key(seed + 1), part), 5)
    prefix, valid = draw_lengths(local[0])
    q_cols = NUM_HEADS * HEAD_DIM
    kv_cols = KV_STORE * HEAD_DIM
    hidden = gauss(local[1], (REQUESTS, CHUNK_LEN, MODEL_DIM), 1.0)
    k_cache = kv_copies(gauss(local[2], (REQUESTS, CACHE_SLOTS, KV_HEADS, HEAD_DIM), 1.0), 2)
    v_mean = gauss(local[3], (REQUESTS, 1, KV_HEADS, HEAD_DIM), 1.0)
    v_cache = kv_copies(v_mean + gauss(local[4], (REQUESTS, CACHE_SLOTS, KV_HEADS, HEAD_DIM), 1.5), 2)
    w_k = kv_copies(gauss(shared[3], (MODEL_DIM, KV_HEADS, HEAD_DIM), MODEL_DIM ** -0.5), 1)
    b_k = kv_copies(gauss(shared[4], (KV_HEADS, HEAD_DIM), 1.0), 0)
    w_v = kv_copies(gauss(shared[5], (MODEL_DIM, KV_HEADS, HEAD_DIM), MODEL_DIM ** -0.5), 1)
    b_v = kv_copies(gauss(shared[6], (KV_HEADS, HEAD_DIM), 1.0), 0)
    return {
        "x": hidden.astype(jnp.bfloat16),
        "k_cache": k_cache.astype(jnp.bfloat16),
        "v_cache": v_cache.astype(jnp.bfloat16),
        "prefix_len": prefix,
        "valid_len": valid,
        "g_attn": (1.0 + gauss(shared[0], (MODEL_DIM,), 0.3)).astype(jnp.bfloat16),
        "w_q": gauss(shared[1], (MODEL_DIM, q_cols), 1.5 * MODEL_DIM ** -0.5).astype(jnp.bfloat16),
        "b_q": gauss(shared[2], (q_cols,), 1.0).astype(jnp.bfloat16),
        "w_k": w_k.reshape(MODEL_DIM, kv_cols).astype(jnp.bfloat16),
        "b_k": b_k.reshape(kv_cols).astype(jnp.bfloat16),
        "w_v": w_v.reshape(MODEL_DIM, kv_cols).astype(jnp.bfloat16),
        "b_v": b_v.reshape(kv_cols).astype(jnp.bfloat16),
        "w_o": gauss(shared[7], (q_cols, MODEL_DIM), q_cols ** -0.5).astype(jnp.bfloat16),
        "g_mlp": (1.0 + gauss(shared[8], (MODEL_DIM,), 0.3)).astype(jnp.bfloat16),
        "w_gate": gauss(shared[9], (MODEL_DIM, FFN_DIM), MODEL_DIM ** -0.5).astype(jnp.bfloat16),
        "w_up": gauss(shared[10], (MODEL_DIM, FFN_DIM), MODEL_DIM ** -0.5).astype(jnp.bfloat16),
        "w_down": gauss(shared[11], (FFN_DIM, MODEL_DIM), 1.5 * FFN_DIM ** -0.5).astype(jnp.bfloat16),
    }


def rms_norm(hidden, gain):
    wide_vals = hidden.astype(jnp.float32)
    inv_rms = lax.rsqrt(jnp.mean(wide_vals * wide_vals, axis=-1, keepdims=True) + NORM_EPS)
    return (wide_vals * inv_rms * gain.astype(jnp.float32)).astype(jnp.bfloat16)


def rotate_heads(heads, positions):
    half = heads.shape[-1] // 2
    inv_freq = ROPE_THETA ** (-(jnp.arange(half, dtype=jnp.float32) * 2.0) / heads.shape[-1])
    angles = positions.astype(jnp.float32)[..., None] * inv_freq
    cos_t = jnp.cos(angles)[..., None, :]
    sin_t = jnp.sin(angles)[..., None, :]
    wide = heads.astype(jnp.float32)
    first_half = wide[..., :half]
    second_half = wide[..., half:]
    rotated = jnp.concatenate([first_half * cos_t - second_half * sin_t, second_half * cos_t + first_half * sin_t], axis=-1)
    return rotated.astype(jnp.bfloat16)


def project(hidden, weight, bias):
    total = jnp.dot(hidden, weight, preferred_element_type=jnp.float32)
    return (total + bias.astype(jnp.float32)).astype(jnp.bfloat16)


def reference(x, k_cache, v_cache, prefix_len, valid_len, g_attn, w_q, b_q, w_k, b_k, w_v, b_v, w_o, g_mlp, w_gate, w_up, w_down):
    row_ids = jnp.arange(CHUNK_LEN)
    slot_ids = jnp.arange(CACHE_SLOTS)

    def one_request(req_args):
        hidden, k_rows, v_rows, start, count = req_args
        positions = start + row_ids
        normed = rms_norm(hidden, g_attn)
        queries = rotate_heads(project(normed, w_q, b_q).reshape(CHUNK_LEN, NUM_HEADS, HEAD_DIM), positions)
        keys_new = rotate_heads(project(normed, w_k, b_k).reshape(CHUNK_LEN, KV_STORE, HEAD_DIM), positions)
        values_new = project(normed, w_v, b_v).reshape(CHUNK_LEN, KV_STORE, HEAD_DIM)
        keep = (row_ids < count)[:, None, None]
        k_old = lax.dynamic_slice_in_dim(k_rows, start, CHUNK_LEN, axis=0)
        v_old = lax.dynamic_slice_in_dim(v_rows, start, CHUNK_LEN, axis=0)
        k_rows = lax.dynamic_update_slice_in_dim(k_rows, jnp.where(keep, keys_new, k_old), start, axis=0)
        v_rows = lax.dynamic_update_slice_in_dim(v_rows, jnp.where(keep, values_new, v_old), start, axis=0)
        limit = start + jnp.minimum(row_ids, count - 1)
        visible = slot_ids[None, :] <= limit[:, None]
        query_groups = queries.reshape(CHUNK_LEN, KV_STORE, GROUP_SIZE, HEAD_DIM)

        def one_head(head_args):
            q_head, k_head, v_head = head_args
            scores = jnp.einsum("cgd,sd->gcs", q_head.astype(jnp.float32), k_head.astype(jnp.float32)) * HEAD_DIM ** -0.5
            scores = jnp.where(visible[None], scores, -1.0e30)
            attn_probs = jax.nn.softmax(scores, axis=-1).astype(jnp.bfloat16)
            mixed = jnp.einsum("gcs,sd->cgd", attn_probs.astype(jnp.float32), v_head.astype(jnp.float32))
            return mixed.astype(jnp.bfloat16)

        heads_out = lax.map(one_head, (jnp.moveaxis(query_groups, 1, 0), jnp.moveaxis(k_rows, 1, 0), jnp.moveaxis(v_rows, 1, 0)))
        attended = jnp.moveaxis(heads_out, 0, 1).reshape(CHUNK_LEN, NUM_HEADS * HEAD_DIM)
        attn_out = jnp.dot(attended, w_o, preferred_element_type=jnp.float32).astype(jnp.bfloat16)
        resid_mid = (hidden.astype(jnp.float32) + attn_out.astype(jnp.float32)).astype(jnp.bfloat16)
        normed_mlp = rms_norm(resid_mid, g_mlp)
        gate = jnp.dot(normed_mlp, w_gate, preferred_element_type=jnp.float32)
        up_proj = jnp.dot(normed_mlp, w_up, preferred_element_type=jnp.float32)
        hidden_act = (jax.nn.silu(gate) * up_proj).astype(jnp.bfloat16)
        down = jnp.dot(hidden_act, w_down, preferred_element_type=jnp.float32).astype(jnp.bfloat16)
        result = (resid_mid.astype(jnp.float32) + down.astype(jnp.float32)).astype(jnp.bfloat16)
        return result, k_rows, v_rows

    x_out, k_out, v_out = lax.map(one_request, (x, k_cache, v_cache, prefix_len, valid_len))
    return x_out, k_out, v_out
```

```python
import functools

import jax
import jax.numpy as jnp
from jax import lax
from jax.experimental import pallas as pl
from jax.experimental.pallas import tpu as pltpu
from jax.sharding import PartitionSpec as P

ROPE_THETA = 1.0e6
NORM_EPS = 1.0e-6
MESH = pl.DeviceIdType.MESH
BF = jnp.bfloat16
F32 = jnp.float32

REQ = 2
ROWS = 64
RANKS = 8
CHUNK = ROWS * RANKS
DIM = 4096
HEADS = 4
HD = 128
SLOTS = 4096
OLD = SLOTS - CHUNK
FFN = 1376


class Place:
    def __init__(self):
        t = lax.axis_index("tp")
        self.me = t
        self.c = t % 2
        self.z = t // 2
        self.half = self.z // 2
        self.zm = self.z + self.half * (3 - 2 * self.z)
        self.away = 2 * (self.z + 1 - 2 * self.half) + self.c
        self.near = 2 * (self.z - 1 + 2 * self.half) + self.c
        self.partner = 2 * self.z + 1 - self.c

    def chip(self, dm):
        return dm + self.half * (3 - 2 * dm)

    def blk(self, dm):
        return 2 * self.chip(dm) + self.c

    def other(self, dm):
        return 2 * self.chip(dm) + 1 - self.c

    def outer(self):
        return self.zm == 0

    def inner(self):
        return self.zm == 1


def entry_barrier(pos):
    bar = pltpu.get_barrier_semaphore()

    def signal(dev):
        pl.semaphore_signal(bar, inc=1, device_id={"tp": dev}, device_id_type=MESH)

    signal(pos.partner)
    signal(pos.away)

    @pl.when(pos.inner())
    def _():
        signal(pos.near)
        pl.semaphore_wait(bar, 3)

    @pl.when(pos.outer())
    def _():
        pl.semaphore_wait(bar, 2)


class Gather:
    def __init__(self, pos, buf, send, recv):
        self.pos, self.buf, self.send, self.recv = pos, buf, send, recv

    def copy(self, t, dev, n):
        ref = self.buf.at[t]
        return pltpu.make_async_remote_copy(
            src_ref=ref, dst_ref=ref, send_sem=self.send.at[n], recv_sem=self.recv.at[t],
            device_id={"tp": dev}, device_id_type=MESH)

    def wait_block(self, t):
        self.copy(t, self.pos.partner, 0).wait_recv()

    def start(self, outer=True, inner=True):
        p = self.pos
        if outer:
            @pl.when(p.outer())
            def _():
                self.copy(p.me, p.away, 0).start()
                self.copy(p.me, p.partner, 1).start()
        if inner:
            @pl.when(p.inner())
            def _():
                self.copy(p.me, p.near, 0).start()
                self.copy(p.me, p.away, 1).start()
                self.copy(p.me, p.partner, 2).start()

    def step(self, i):
        p = self.pos

        @pl.when(p.outer())
        def _():
            t = p.blk(i)
            self.wait_block(t)
            self.copy(t, p.partner, 1 + i).start()

        if i == 1:
            @pl.when(p.inner())
            def _():
                t = p.blk(0)
                self.wait_block(t)
                self.copy(t, p.away, 3).start()
                self.copy(t, p.partner, 4).start()
                t = p.blk(2)
                self.wait_block(t)
                self.copy(t, p.near, 5).start()
                self.copy(t, p.partner, 6).start()
        if i == 2:
            @pl.when(p.inner())
            def _():
                t = p.blk(3)
                self.wait_block(t)
                self.copy(t, p.near, 7).start()
                self.copy(t, p.partner, 8).start()

    def finish(self):
        for dm in range(4):
            self.wait_block(self.pos.other(dm))

    def drain(self):
        p = self.pos

        @pl.when(p.outer())
        def _():
            for n in range(5):
                self.copy(p.me, p.partner, n).wait_send()

        @pl.when(p.inner())
        def _():
            for n in range(9):
                self.copy(p.me, p.partner, n).wait_send()


def row_loop(body):
    def run(i, carry):
        body(pl.ds(pl.multiple_of(i * 16, 16), 16))
        return carry

    lax.fori_loop(0, ROWS // 16, run, 0)


class Scatter:
    def __init__(self, pos, part, prx, near, far, psend, precv, send, nrecv, frecv):
        self.pos, self.part, self.prx, self.near, self.far = pos, part, prx, near, far
        self.psend, self.precv, self.send, self.nrecv, self.frecv = psend, precv, send, nrecv, frecv

    def to_partner(self, dm):
        p = self.pos
        return pltpu.make_async_remote_copy(
            src_ref=self.part.at[p.other(dm)], dst_ref=self.prx.at[dm], send_sem=self.psend.at[dm],
            recv_sem=self.precv.at[dm], device_id={"tp": p.partner}, device_id_type=MESH)

    def hop(self, dm, dev, dst, recv):
        return pltpu.make_async_remote_copy(
            src_ref=self.part.at[self.pos.blk(dm)], dst_ref=dst, send_sem=self.send.at[dm],
            recv_sem=recv, device_id={"tp": dev}, device_id_type=MESH)

    def hop_near(self, dm, dev):
        return self.hop(dm, dev, self.near.at[dm - 1], self.nrecv.at[dm - 1])

    def hop_far(self, dm, dev, slot):
        return self.hop(dm, dev, self.far.at[slot], self.frecv.at[slot])

    def swap(self):
        for dm in (3, 2, 1, 0):
            self.to_partner(dm).start()

    def add(self, dm, *more):
        dst = self.part.at[self.pos.blk(dm)]

        def body(rows):
            total = dst[rows, :].astype(F32) + self.prx[dm, rows, :].astype(F32)
            for ref in more:
                total = total + ref[rows, :].astype(F32)
            dst[rows, :] = total.astype(BF)

        row_loop(body)

    def outer_sends(self):
        p = self.pos

        @pl.when(p.outer())
        def _():
            for dm in (3, 2, 1):
                self.to_partner(dm).wait_recv()
                self.add(dm)
                self.hop_near(dm, p.away).start()

    def inner_step(self, i):
        p = self.pos

        @pl.when(p.inner())
        def _():
            if i == 1:
                self.to_partner(3).wait_recv()
                self.hop_near(3, p.away).wait_recv()
                self.add(3, self.near.at[2])
                self.hop_far(3, p.away, 0).start()
            if i == 2:
                self.to_partner(2).wait_recv()
                self.hop_near(2, p.away).wait_recv()
                self.add(2, self.near.at[1])
                self.hop_far(2, p.away, 1).start()
            if i == 3:
                self.to_partner(0).wait_recv()
                self.hop_far(0, p.near, 0).wait_recv()
                self.add(0, self.far.at[0])
                self.hop_far(0, p.near, 0).start()

    def final(self, use):
        p = self.pos

        @pl.when(p.outer())
        def _():
            self.to_partner(0).wait_recv()
            self.hop_far(0, p.near, 0).wait_recv()
            use((self.part.at[p.blk(0)], self.prx.at[0], self.far.at[0]))

        @pl.when(p.inner())
        def _():
            self.to_partner(1).wait_recv()
            self.hop_near(1, p.away).wait_recv()
            self.hop_far(1, p.away, 1).wait_recv()
            use((self.part.at[p.blk(1)], self.prx.at[1], self.near.at[0], self.far.at[1]))

    def drain(self):
        p = self.pos
        for dm in range(4):
            self.to_partner(dm).wait_send()

        @pl.when(p.outer())
        def _():
            for dm in (3, 2, 1):
                self.hop_near(dm, p.away).wait_send()

        @pl.when(p.inner())
        def _():
            for dm in (3, 2, 0):
                self.hop_far(dm, p.away, 0).wait_send()


def norm_value(wide, gain):
    inv_rms = lax.rsqrt(jnp.mean(wide * wide, axis=-1, keepdims=True) + NORM_EPS)
    return (wide * inv_rms * gain).astype(BF)


RELAY = 256
N_RELAY = REQ * OLD // RELAY


def qkv_kernel(pre_ref, x_ref, g_ref, bq_ref, bk_ref, bv_ref, kc_ref, vc_ref, wq_hbm, wk_hbm, wv_hbm,
               q_out, k_out, v_out, kn_out, vn_out, kh_out, vh_out,
               hbuf, wbuf, obuf, rbuf, cosb, sinb, cin, wide, cout,
               wsem, osem, rsem, isem, csem, gsend, grecv):
    pos = Place()
    weights = [pltpu.make_async_copy(src, wbuf.at[i], wsem.at[i]) for i, src in enumerate((wq_hbm, wk_hbm, wv_hbm))]
    for cp in weights:
        cp.start()
    gain = g_ref[...].astype(F32)
    gathers = [Gather(pos, hbuf.at[r], gsend.at[r], grecv.at[r]) for r in range(REQ)]

    per_req = OLD // RELAY
    srcs = (kc_ref, vc_ref)
    dsts = (kh_out, vh_out)

    def fetch(n, w, slot):
        return pltpu.make_async_copy(
            srcs[w].at[n // per_req, pl.ds(pl.multiple_of((n % per_req) * RELAY * HEADS, RELAY * HEADS), RELAY * HEADS)],
            cin.at[slot, w], isem.at[slot, w])

    def flush(n, w, slot):
        return pltpu.make_async_copy(
            cout.at[slot, w],
            dsts[w].at[n // per_req, :, pl.ds(pl.multiple_of((n % per_req) * RELAY, RELAY), RELAY)],
            csem.at[slot, w])

    for w in range(2):
        fetch(0, w, 0).start()

    def norm_rows(r):
        def body(rows):
            hbuf[r, pos.me, rows, :] = norm_value(x_ref[r, rows, :].astype(F32), gain)

        row_loop(body)

    norm_rows(0)
    entry_barrier(pos)
    gathers[0].start()
    norm_rows(1)
    gathers[1].start(inner=False)

    def relay(n, carry):
        slot = n % 2
        for w in range(2):
            @pl.when(n + 1 < N_RELAY)
            def _():
                fetch(n + 1, w, 1 - slot).start()

            fetch(n, w, slot).wait()

            @pl.when(n >= 2)
            def _():
                flush(n - 2, w, slot).wait()

            wide[w] = cin[slot, w].astype(F32)
            for h in range(HEADS):
                cout[slot, w, h] = wide[w, pl.ds(h, RELAY, stride=HEADS), :].astype(BF)
            flush(n, w, slot).start()
        return carry

    third = N_RELAY // 3
    lax.fori_loop(0, third, relay, 0)
    gathers[0].step(1)
    lax.fori_loop(third, 2 * third, relay, 0)
    gathers[0].step(2)
    gathers[1].start(outer=False)

    half = HD // 2
    lane = lax.broadcasted_iota(jnp.int32, (1, HD), 1)
    freq_id = (lane % half).astype(F32)
    inv_freq = jnp.exp((freq_id * 2.0 / HD) * (-jnp.log(jnp.float32(ROPE_THETA))))
    sign = jnp.where(lane < half, -1.0, 1.0).astype(F32)
    row_pos = lax.broadcasted_iota(jnp.int32, (CHUNK, 1), 0)
    for r in range(REQ):
        angles = (row_pos + pre_ref[r]).astype(F32) * inv_freq
        cosb[r] = jnp.cos(angles)
        sinb[r] = jnp.sin(angles) * sign

    lax.fori_loop(2 * third, N_RELAY, relay, 0)
    for n in (N_RELAY - 2, N_RELAY - 1):
        for w in range(2):
            flush(n, w, n % 2).wait()
    gathers[0].step(3)
    gathers[0].finish()
    for cp in weights:
        cp.wait()

    biases = (bq_ref, bk_ref, bv_ref)
    outs = (q_out, k_out, v_out)

    def head_out(i, r):
        return pltpu.make_async_copy(obuf.at[i, r], outs[i].at[r], osem.at[i, r])

    def row_out(i, r):
        return pltpu.make_async_copy(rbuf.at[i - 1, r], (kn_out, vn_out)[i - 1].at[r], rsem.at[i - 1, r])

    def project(i, r):
        for tile in range(2):
            cols = slice(tile * 256, tile * 256 + 256)
            acc = jnp.dot(hbuf[r].reshape(CHUNK, DIM), wbuf[i, :, cols], preferred_element_type=F32)
            val = (acc + biases[i][:, cols].astype(F32)).astype(BF)
            for k in range(2):
                h = tile * 2 + k
                head = val[:, k * HD:(k + 1) * HD]
                if i < 2:
                    wide_head = head.astype(F32)
                    head = (wide_head * cosb[r] + pltpu.roll(wide_head, half, 1) * sinb[r]).astype(BF)
                obuf[i, r, h] = head
                if i > 0:
                    rbuf[i - 1, r, :, h * HD:(h + 1) * HD] = head
        head_out(i, r).start()
        if i > 0:
            row_out(i, r).start()

    for i in range(3):
        project(i, 0)
        gathers[1].step(i + 1)
    gathers[1].finish()
    for i in range(3):
        project(i, 1)
    for r in range(REQ):
        gathers[r].drain()
        for i in range(3):
            head_out(i, r).wait()
            if i > 0:
                row_out(i, r).wait()


def run_qkv(x_rows, k_flat, v_flat, prefix, g, w_q, b_q, w_k, b_k, w_v, b_v):
    vm = pl.BlockSpec(memory_space=pltpu.VMEM)
    sm = pl.BlockSpec(memory_space=pltpu.SMEM)
    anyspace = pl.BlockSpec(memory_space=pl.ANY)
    head = jax.ShapeDtypeStruct((REQ, HEADS, CHUNK, HD), BF)
    rows = jax.ShapeDtypeStruct((REQ, CHUNK, HEADS * HD), BF)
    old = jax.ShapeDtypeStruct((REQ, HEADS, OLD, HD), BF)
    dma = pltpu.SemaphoreType.DMA
    return pl.pallas_call(
        qkv_kernel,
        out_shape=(head, head, head, rows, rows, old, old),
        in_specs=[sm, vm, vm, vm, vm, vm] + [anyspace] * 5,
        out_specs=[anyspace] * 7,
        scratch_shapes=[
            pltpu.VMEM((REQ, RANKS, ROWS, DIM), BF),
            pltpu.VMEM((3, DIM, HEADS * HD), BF),
            pltpu.VMEM((3, REQ, HEADS, CHUNK, HD), BF),
            pltpu.VMEM((2, REQ, CHUNK, HEADS * HD), BF),
            pltpu.VMEM((REQ, CHUNK, HD), F32),
            pltpu.VMEM((REQ, CHUNK, HD), F32),
            pltpu.VMEM((2, 2, RELAY * HEADS, HD), BF),
            pltpu.VMEM((2, RELAY * HEADS, HD), F32),
            pltpu.VMEM((2, 2, HEADS, RELAY, HD), BF),
            dma((3,)), dma((3, REQ)), dma((2, REQ)), dma((2, 2)), dma((2, 2)),
            dma((REQ, 9)), dma((REQ, RANKS)),
        ],
        compiler_params=pltpu.CompilerParams(collective_id=0, has_side_effects=True, vmem_limit_bytes=60 << 20),
        name="gather_qkv",
    )(prefix, x_rows, g.reshape(1, DIM), b_q.reshape(1, -1), b_k.reshape(1, -1), b_v.reshape(1, -1),
      k_flat, v_flat, w_q, w_k, w_v)


KB = 512
COPY = 512
N_COPY = REQ * SLOTS // COPY
STEPS = REQ * HEADS
PER_STEP = N_COPY // STEPS


def attn_kernel(pre_ref, val_ref, q_ref, ko_ref, vo_ref, kn_ref, vn_ref, kc_hbm, vc_hbm, krow_hbm, vrow_hbm,
                o_ref, kout_hbm, vout_hbm, cbuf, nbuf, isem, osem, nsem, usem):
    r = pl.program_id(0)
    h = pl.program_id(1)
    step = r * HEADS + h
    srcs = (kc_hbm, vc_hbm)
    dsts = (kout_hbm, vout_hbm)
    news = (krow_hbm, vrow_hbm)

    def chunk(s, j):
        n = s * PER_STEP + j
        return n // (SLOTS // COPY), pl.ds((n % (SLOTS // COPY)) * COPY, COPY)

    def take(s, j, w):
        i, rows = chunk(s, j)
        return pltpu.make_async_copy(srcs[w].at[i, rows], cbuf.at[s % 2, j, w], isem.at[s % 2, j, w])

    def put(s, j, w):
        i, rows = chunk(s, j)
        return pltpu.make_async_copy(cbuf.at[s % 2, j, w], dsts[w].at[i, rows], osem.at[s % 2, j, w])

    def each(fn):
        for j in range(PER_STEP):
            for w in range(2):
                fn(j, w)

    @pl.when(step == 0)
    def _():
        each(lambda j, w: take(0, j, w).start())
        for w in range(2):
            pltpu.make_async_copy(news[w], nbuf.at[w], nsem.at[w]).start()

    each(lambda j, w: take(step, j, w).wait())
    each(lambda j, w: put(step, j, w).start())

    @pl.when(step >= 1)
    def _():
        each(lambda j, w: put(step - 1, j, w).wait())

    @pl.when(step + 1 < STEPS)
    def _():
        each(lambda j, w: take(step + 1, j, w).start())

    p = pre_ref[r]
    c = val_ref[r]
    q = q_ref[0, 0]
    scale = (HD ** -0.5) * 1.4426950408889634

    def scores(keys):
        return lax.dot_general(q, keys, (((1,), (1,)), ((), ())), preferred_element_type=F32) * scale

    def fold(carry, s, vals):
        m, l, acc = carry
        m_new = jnp.maximum(m, jnp.max(s, axis=-1, keepdims=True))
        shrink = jnp.exp2(m - m_new)
        probs = jnp.exp2(s - m_new)
        l = l * shrink + jnp.sum(probs, axis=-1, keepdims=True)
        acc = acc * shrink + jnp.dot(probs.astype(BF), vals, preferred_element_type=F32)
        return m_new, l, acc

    rows = lax.broadcasted_iota(jnp.int32, (CHUNK, CHUNK), 0)
    cols = lax.broadcasted_iota(jnp.int32, (CHUNK, CHUNK), 1)
    s = jnp.where(cols <= jnp.minimum(rows, c - 1), scores(kn_ref[0, 0]), -1.0e30)
    m = jnp.max(s, axis=-1, keepdims=True)
    probs = jnp.exp2(s - m)
    l = jnp.sum(probs, axis=-1, keepdims=True)
    acc = jnp.dot(probs.astype(BF), vn_ref[0, 0], preferred_element_type=F32)

    def full(b, carry):
        rows = pl.ds(pl.multiple_of(b * KB, KB), KB)
        return fold(carry, scores(ko_ref[0, 0, rows, :]), vo_ref[0, 0, rows, :])

    def partial(b, carry):
        rows = pl.ds(pl.multiple_of(b * KB, KB), KB)
        s = jnp.where(cols + b * KB < p, scores(ko_ref[0, 0, rows, :]), -1.0e30)
        return fold(carry, s, vo_ref[0, 0, rows, :])

    n_full = p // KB
    n_all = (p + KB - 1) // KB
    carry = lax.fori_loop(0, n_full, full, (m, l, acc))
    m, l, acc = lax.fori_loop(n_full, n_all, partial, carry)
    o_ref[0] = (acc / l).astype(BF)

    @pl.when(step == STEPS - 1)
    def _():
        each(lambda j, w: put(step, j, w).wait())
        for w in range(2):
            pltpu.make_async_copy(news[w], nbuf.at[w], nsem.at[w]).wait()

        def updates(act):
            for i in range(REQ):
                n = val_ref[i]
                for bit in range(10):
                    size = 1 << bit
                    first = (n >> (bit + 1)) << (bit + 1)

                    @pl.when((n >> bit) % 2 == 1)
                    def _():
                        for w in range(2):
                            act(pltpu.make_async_copy(
                                nbuf.at[w, i, pl.ds(first, size)],
                                dsts[w].at[i, pl.ds(pre_ref[i] + first, size)],
                                usem.at[w, i, bit]))

        updates(lambda cp: cp.start())
        updates(lambda cp: cp.wait())


def run_attn(prefix, valid, q, k_old, v_old, k_new, v_new, k_cache, v_cache, k_rows, v_rows):
    def per_head(n):
        return pl.BlockSpec((1, 1, n, HD), lambda r, h, *_: (r, h, 0, 0))

    anyspace = pl.BlockSpec(memory_space=pl.ANY)
    dma = pltpu.SemaphoreType.DMA
    cache = jax.ShapeDtypeStruct((REQ, SLOTS, HEADS, HD), BF)
    return pl.pallas_call(
        attn_kernel,
        out_shape=(jax.ShapeDtypeStruct((REQ, CHUNK, HEADS * HD), BF), cache, cache),
        grid_spec=pltpu.PrefetchScalarGridSpec(
            num_scalar_prefetch=2,
            grid=(REQ, HEADS),
            in_specs=[per_head(CHUNK), per_head(OLD), per_head(OLD), per_head(CHUNK), per_head(CHUNK)] + [anyspace] * 4,
            out_specs=[pl.BlockSpec((1, CHUNK, HD), lambda r, h, *_: (r, 0, h)), anyspace, anyspace],
            scratch_shapes=[
                pltpu.VMEM((2, PER_STEP, 2, COPY, HEADS, HD), BF),
                pltpu.VMEM((2, REQ, CHUNK, HEADS, HD), BF),
                dma((2, PER_STEP, 2)), dma((2, PER_STEP, 2)), dma((2,)), dma((2, REQ, 10)),
            ],
        ),
        compiler_params=pltpu.CompilerParams(dimension_semantics=("arbitrary", "arbitrary"), vmem_limit_bytes=60 << 20),
        name="attend",
    )(prefix, valid, q, k_old, v_old, k_new, v_new, k_cache, v_cache, k_rows, v_rows)


FT = 256
N_FULL = FFN // FT
TAIL = FFN - N_FULL * FT
OT = 512


def mlp_kernel(x_ref, g_ref, o_hbm, wo_hbm, wg_hbm, wu_hbm, wd_hbm, out_ref,
               obuf, wo, wd, wgu, hbuf, ubuf, part, prx, near, far, mid,
               lsem, wsem, gsend, grecv, psend, precv, send, nrecv, frecv):
    pos = Place()
    loads = [pltpu.make_async_copy(src, dst, lsem.at[i]) for i, (src, dst) in enumerate(((o_hbm, obuf), (wo_hbm, wo), (wd_hbm, wd)))]
    for cp in loads:
        cp.start()

    def fetch(tile, slot, size):
        rows = pl.ds(pl.multiple_of(tile * FT, FT), size)
        return [pltpu.make_async_copy(src.at[rows], wgu.at[slot, w, pl.ds(0, size)], wsem.at[slot, w])
                for w, src in enumerate((wg_hbm, wu_hbm))]

    for cp in fetch(0, 0, FT):
        cp.start()
    gain = g_ref[...].astype(F32)
    gathers = [Gather(pos, hbuf.at[r], gsend.at[r], grecv.at[r]) for r in range(REQ)]
    scat = [[Scatter(pos, part.at[r], prx.at[r], near.at[r], far.at[r], psend.at[k, r], precv.at[k, r],
                     send.at[k, r], nrecv.at[k, r], frecv.at[k, r]) for r in range(REQ)] for k in range(2)]

    def into_part(r, lhs, weight):
        def tile(n, carry):
            cols = pl.ds(pl.multiple_of(n * OT, OT), OT)
            res = jnp.dot(lhs(), weight[:, cols], preferred_element_type=F32).astype(BF)
            part[r, :, :, cols] = res.reshape(RANKS, ROWS, OT)
            return carry

        lax.fori_loop(0, DIM // OT, tile, 0)

    def mid_rows(r):
        def use(refs):
            def body(rows):
                total = refs[0][rows, :].astype(F32)
                for ref in refs[1:]:
                    total = total + ref[rows, :].astype(F32)
                x1 = (x_ref[r, rows, :].astype(F32) + total.astype(BF).astype(F32)).astype(BF)
                mid[r, rows, :] = x1
                hbuf[r, pos.me, rows, :] = norm_value(x1.astype(F32), gain)

            row_loop(body)

        return use

    def out_rows(r):
        def use(refs):
            def body(rows):
                total = refs[0][rows, :].astype(F32)
                for ref in refs[1:]:
                    total = total + ref[rows, :].astype(F32)
                out_ref[r, rows, :] = (mid[r, rows, :].astype(F32) + total.astype(BF).astype(F32)).astype(BF)

            row_loop(body)

        return use

    def act(r, slot, size):
        dims = (((1,), (1,)), ((), ()))
        h = hbuf[r].reshape(CHUNK, DIM)
        gate = lax.dot_general(h, wgu[slot, 0, :size], dims, preferred_element_type=F32)
        up = lax.dot_general(h, wgu[slot, 1, :size], dims, preferred_element_type=F32)
        return (gate * (1.0 / (1.0 + jnp.exp(-gate))) * up).astype(BF)

    def mlp_up(r):
        def tile(n, carry):
            slot = n % 2
            for cp in fetch(n, slot, FT):
                cp.wait()

            @pl.when(n + 1 < N_FULL)
            def _():
                for cp in fetch(n + 1, 1 - slot, FT):
                    cp.start()

            @pl.when(n + 1 == N_FULL)
            def _():
                for cp in fetch(N_FULL, 1 - slot, TAIL):
                    cp.start()

            ubuf[:, pl.ds(pl.multiple_of(n * FT, FT), FT)] = act(r, slot, FT)
            return carry

        lax.fori_loop(0, N_FULL, tile, 0)
        slot = N_FULL % 2
        for cp in fetch(N_FULL, slot, TAIL):
            cp.wait()
        if r + 1 < REQ:
            for cp in fetch(0, 1 - slot, FT):
                cp.start()
        ubuf[:, N_FULL * FT:] = act(r, slot, TAIL)

    entry_barrier(pos)
    loads[0].wait()
    loads[1].wait()
    for r in range(REQ):
        into_part(r, lambda: obuf[r], wo)
        scat[0][r].swap()
        scat[0][r].outer_sends()
    for i in (1, 2, 3):
        scat[0][0].inner_step(i)
    scat[0][0].final(mid_rows(0))
    gathers[0].start()
    scat[0][1].inner_step(1)
    gathers[0].step(1)
    scat[0][1].inner_step(2)
    gathers[0].step(2)
    scat[0][1].inner_step(3)
    scat[0][1].final(mid_rows(1))
    gathers[0].step(3)
    gathers[1].start()
    gathers[0].finish()
    loads[2].wait()
    for r in range(REQ):
        mlp_up(r)
        if r == 0:
            gathers[1].step(1)
        gathers[r].drain()
        scat[0][r].drain()
        into_part(r, lambda: ubuf[...], wd)
        scat[1][r].swap()
        scat[1][r].outer_sends()
        if r == 0:
            gathers[1].step(2)
            gathers[1].step(3)
            gathers[1].finish()
            for i in (1, 2, 3):
                scat[1][0].inner_step(i)
    scat[1][0].final(out_rows(0))
    for i in (1, 2, 3):
        scat[1][1].inner_step(i)
    scat[1][1].final(out_rows(1))
    for r in range(REQ):
        scat[1][r].drain()


def run_mlp(x_rows, attended, g, w_o, w_gate_t, w_up_t, w_down):
    vm = pl.BlockSpec(memory_space=pltpu.VMEM)
    anyspace = pl.BlockSpec(memory_space=pl.ANY)
    dma = pltpu.SemaphoreType.DMA
    block = (ROWS, DIM)
    return pl.pallas_call(
        mlp_kernel,
        out_shape=jax.ShapeDtypeStruct((REQ, ROWS, DIM), BF),
        in_specs=[vm, vm] + [anyspace] * 5,
        out_specs=vm,
        scratch_shapes=[
            pltpu.VMEM((REQ, CHUNK, HEADS * HD), BF),
            pltpu.VMEM((HEADS * HD, DIM), BF),
            pltpu.VMEM((FFN, DIM), BF),
            pltpu.VMEM((2, 2, FT, DIM), BF),
            pltpu.VMEM((REQ, RANKS) + block, BF),
            pltpu.VMEM((CHUNK, FFN), BF),
            pltpu.VMEM((REQ, RANKS) + block, BF),
            pltpu.VMEM((REQ, 4) + block, BF),
            pltpu.VMEM((REQ, 3) + block, BF),
            pltpu.VMEM((REQ, 2) + block, BF),
            pltpu.VMEM((REQ,) + block, BF),
            dma((3,)), dma((2, 2)), dma((REQ, 9)), dma((REQ, RANKS)),
            dma((2, REQ, 4)), dma((2, REQ, 4)), dma((2, REQ, 4)), dma((2, REQ, 3)), dma((2, REQ, 2)),
        ],
        compiler_params=pltpu.CompilerParams(collective_id=1, has_side_effects=True, vmem_limit_bytes=63 << 20),
        name="out_mlp",
    )(x_rows, g.reshape(1, DIM), attended, w_o, w_gate_t, w_up_t, w_down)


def solution(mesh):
    row_spec = P("dp", "tp", None)
    cache_spec = P("dp", None, "tp", None)
    req_spec = P("dp")
    rep_spec = P(None)
    col_spec = P(None, "tp")
    bias_spec = P("tp")
    down_spec = P("tp", None)

    def layer(x_rows, k_cache, v_cache, prefix, valid, g_attn, w_q, b_q, w_k, b_k, w_v, b_v, w_o, g_mlp, w_gate, w_up, w_down):
        flat = (REQ, SLOTS * HEADS, HD)
        q, k_new, v_new, k_rows, v_rows, k_old, v_old = run_qkv(
            x_rows, k_cache.reshape(flat), v_cache.reshape(flat), prefix, g_attn, w_q, b_q, w_k, b_k, w_v, b_v)
        wide = (REQ, CHUNK, HEADS, HD)
        attended, k_out, v_out = run_attn(
            prefix, valid, q, k_old, v_old, k_new, v_new, k_cache, v_cache, k_rows.reshape(wide), v_rows.reshape(wide))
        x_out = run_mlp(x_rows, attended, g_mlp, w_o, w_gate.T, w_up.T, w_down)
        return x_out, k_out, v_out

    in_specs = (row_spec, cache_spec, cache_spec, req_spec, req_spec, rep_spec, col_spec, bias_spec, col_spec, bias_spec, col_spec, bias_spec, down_spec, rep_spec, col_spec, col_spec, down_spec)
    return jax.shard_map(layer, mesh=mesh, in_specs=in_specs, out_specs=(row_spec, cache_spec, cache_spec), check_vma=False)
```

```python
import jax
import jax.numpy as jnp
from jax import lax
from jax.experimental import pallas as pl
from jax.experimental.pallas import tpu as pltpu
from jax.sharding import PartitionSpec as P

ROPE_THETA = 1.0e6
NORM_EPS = 1.0e-6
MESH = pl.DeviceIdType.MESH
BF = jnp.bfloat16
F32 = jnp.float32

REQ = 2
ROWS = 64
RANKS = 8
CHUNK = ROWS * RANKS
DIM = 4096
HEADS = 4
HD = 128
QKV = HEADS * HD
SLOTS = 4096
OLD = SLOTS - CHUNK
FFN = 1376
PARTS = 2
UNITS = REQ * PARTS
UROWS = ROWS // PARTS
ULEN = CHUNK // PARTS

ORDER = (
    ('pre',), ('a1', 0, 0, 1), ('a1', 0, 0, 0), ('pre2',), ('a1', 1, 0, 0), ('rl', 0), ('a1', 0, 1, 1),
    ('a1', 0, 2, 1), ('cs',), ('rl', 1), ('a1', 0, 1, 0), ('a1', 0, 3, 1), ('a1', 0, 4, 1), ('a1', 0, 2, 0),
    ('rl', 2), ('a1', 0, 3, 0), ('a1', 0, 4, 0), ('a1', 1, 0, 1), ('qkv', 0, 0), ('qkv', 0, 1), ('qkv', 0, 2),
    ('a1', 1, 1, 1), ('a1', 1, 2, 1), ('at', 0, 0), ('a1', 1, 1, 0), ('a1', 1, 3, 1), ('at', 0, 1), ('wo', 0),
    ('sw1', 0, 0), ('a1', 1, 2, 0), ('st1', 0, 1, 0), ('wo', 1), ('sw1', 0, 1), ('st1', 0, 2, 0), ('a1', 1, 4, 1),
    ('sw1', 1, 0), ('st1', 0, 3, 0), ('a1', 1, 3, 0), ('st1', 0, 1, 1), ('st1', 0, 2, 1), ('a1', 1, 4, 0),
    ('qkv', 1, 0), ('qkv', 1, 1), ('st1', 1, 1, 0), ('st1', 0, 3, 1), ('qkv', 1, 2), ('fi1', 0, 1), ('a2', 0, 0, 1),
    ('sw1', 1, 1), ('st1', 1, 1, 1), ('st1', 1, 2, 0), ('at', 1, 0), ('fi1', 0, 0), ('a2', 0, 0, 0),
    ('st1', 1, 2, 1), ('st1', 1, 3, 0), ('at', 1, 1), ('wo', 2), ('sw1', 2, 0), ('a2', 0, 1, 1), ('a2', 0, 2, 1),
    ('wo', 3), ('st1', 1, 3, 1), ('fi1', 1, 1), ('sw1', 3, 0), ('a2', 0, 1, 0), ('st1', 2, 1, 0), ('sw1', 2, 1),
    ('a2', 1, 0, 1), ('st1', 2, 1, 1), ('st1', 2, 2, 0), ('a2', 0, 2, 0), ('sw1', 3, 1), ('st1', 3, 1, 0),
    ('st1', 2, 3, 0), ('st1', 3, 2, 0), ('a2', 0, 3, 1), ('st1', 2, 2, 1), ('st1', 2, 3, 1), ('a2', 0, 3, 0),
    ('st1', 3, 1, 1), ('fi1', 1, 0), ('a2', 0, 4, 1), ('a2', 0, 4, 0), ('fi1', 2, 1), ('a2', 2, 0, 1),
    ('st1', 3, 2, 1), ('st1', 3, 3, 1), ('up', 0, 0), ('a2', 1, 0, 0), ('fi1', 2, 0), ('a2', 2, 0, 0),
    ('a2', 1, 1, 0), ('st1', 3, 3, 0), ('a2', 1, 1, 1), ('up', 0, 1), ('up', 0, 2), ('a2', 1, 2, 1), ('dn', 0, 0),
    ('dn', 0, 1), ('sw2', 0, 0), ('a2', 1, 3, 1), ('st2', 0, 1, 0), ('a2', 2, 1, 1), ('sw2', 0, 1), ('fi1', 3, 0),
    ('a2', 3, 0, 0), ('a2', 2, 2, 1), ('a2', 1, 2, 0), ('st2', 0, 2, 0), ('st2', 0, 3, 0), ('a2', 1, 3, 0),
    ('a2', 2, 1, 0), ('a2', 1, 4, 0), ('fi1', 3, 1), ('a2', 1, 4, 1), ('up', 1, 0), ('up', 1, 1), ('up', 1, 2),
    ('a2', 2, 3, 1), ('a2', 2, 2, 0), ('a2', 3, 0, 1), ('dn', 1, 0), ('a2', 3, 1, 1), ('a2', 2, 4, 1),
    ('st2', 0, 1, 1), ('a2', 2, 3, 0), ('dn', 1, 1), ('sw2', 1, 0), ('a2', 3, 2, 1), ('a2', 2, 4, 0),
    ('st2', 0, 2, 1), ('sw2', 1, 1), ('up', 2, 0), ('a2', 3, 3, 1), ('st2', 1, 1, 0), ('a2', 3, 4, 1), ('up', 2, 1),
    ('st2', 1, 2, 0), ('a2', 3, 1, 0), ('up', 2, 2), ('a2', 3, 2, 0), ('dn', 2, 0), ('dn', 2, 1), ('st2', 1, 3, 0),
    ('a2', 3, 3, 0), ('sw2', 2, 0), ('a2', 3, 4, 0), ('up', 3, 0), ('st2', 1, 1, 1), ('st2', 2, 1, 0),
    ('st2', 2, 2, 0), ('sw2', 2, 1), ('st2', 0, 3, 1), ('up', 3, 1), ('st2', 1, 2, 1), ('up', 3, 2), ('dn', 3, 0),
    ('dn', 3, 1), ('sw2', 3, 1), ('st2', 1, 3, 1), ('sw2', 3, 0), ('fi2', 0, 0), ('st2', 2, 1, 1), ('st2', 3, 1, 0),
    ('st2', 2, 2, 1), ('st2', 2, 3, 1), ('fi2', 0, 1), ('st2', 3, 2, 0), ('fi2', 1, 0), ('fi2', 1, 1),
    ('st2', 3, 1, 1), ('st2', 3, 2, 1), ('st2', 2, 3, 0), ('st2', 3, 3, 0), ('fi2', 2, 0), ('st2', 3, 3, 1),
    ('fi2', 2, 1), ('fi2', 3, 1), ('fi2', 3, 0),
)


class Place:
    def __init__(self):
        t = lax.axis_index("tp")
        self.me = t
        self.c = t % 2
        self.z = t // 2
        self.half = self.z // 2
        self.zm = self.z + self.half * (3 - 2 * self.z)
        self.away = 2 * (self.z + 1 - 2 * self.half) + self.c
        self.near = 2 * (self.z - 1 + 2 * self.half) + self.c
        self.partner = 2 * self.z + 1 - self.c

    def chip(self, dm):
        return dm + self.half * (3 - 2 * dm)

    def blk(self, dm):
        return 2 * self.chip(dm) + self.c

    def other(self, dm):
        return 2 * self.chip(dm) + 1 - self.c

    def role(self, q, fn):
        @pl.when(self.zm == q)
        def _():
            fn()


def entry_barrier(pos):
    bar = pltpu.get_barrier_semaphore()

    def signal(dev):
        pl.semaphore_signal(bar, inc=1, device_id={"tp": dev}, device_id_type=MESH)

    signal(pos.partner)
    signal(pos.away)

    def inner():
        signal(pos.near)
        pl.semaphore_wait(bar, 3)

    pos.role(1, inner)
    pos.role(0, lambda: pl.semaphore_wait(bar, 2))


class Gather:
    def __init__(self, pos, block, send, recv):
        self.pos, self.block, self.send, self.recv = pos, block, send, recv

    def copy(self, t, dev, n):
        ref = self.block(t)
        return pltpu.make_async_remote_copy(
            src_ref=ref, dst_ref=ref, send_sem=self.send(n), recv_sem=self.recv(t),
            device_id={"tp": dev}, device_id_type=MESH)

    def wait_block(self, t):
        self.copy(t, self.pos.partner, 0).wait_recv()

    def step(self, i, q):
        p = self.pos
        if i == 0:
            devs = (p.near, p.away, p.partner) if q else (p.away, p.partner)
            for n, dev in enumerate(devs):
                self.copy(p.me, dev, n).start()
        elif i < 4:
            t = p.blk((0, 2, 3)[i - 1] if q else i)
            self.wait_block(t)
            if q:
                self.copy(t, p.away if i == 1 else p.near, 1 + 2 * i).start()
                self.copy(t, p.partner, 2 + 2 * i).start()
            else:
                self.copy(t, p.partner, 1 + i).start()
        else:
            for dm in range(4):
                self.wait_block(p.other(dm))

    def drain(self):
        p = self.pos

        def wait(count):
            for n in range(count):
                self.copy(p.me, p.partner, n).wait_send()

        p.role(0, lambda: wait(5))
        p.role(1, lambda: wait(9))


def row_loop(body):
    def run(i, carry):
        body(pl.multiple_of(i * 16, 16))
        return carry

    lax.fori_loop(0, UROWS // 16, run, 0)


class Scatter:
    def __init__(self, pos, part, prx, near, far, psend, precv, send, nrecv, frecv):
        self.pos, self.part, self.prx, self.near, self.far = pos, part, prx, near, far
        self.psend, self.precv, self.send, self.nrecv, self.frecv = psend, precv, send, nrecv, frecv

    def to_partner(self, dm):
        p = self.pos
        return pltpu.make_async_remote_copy(
            src_ref=self.part(p.other(dm)), dst_ref=self.prx(dm), send_sem=self.psend(dm),
            recv_sem=self.precv(dm), device_id={"tp": p.partner}, device_id_type=MESH)

    def hop(self, dm, dev, dst, recv):
        return pltpu.make_async_remote_copy(
            src_ref=self.part(self.pos.blk(dm)), dst_ref=dst, send_sem=self.send(dm),
            recv_sem=recv, device_id={"tp": dev}, device_id_type=MESH)

    def hop_near(self, dm, dev):
        return self.hop(dm, dev, self.near(dm - 1), self.nrecv(dm - 1))

    def hop_far(self, dm, dev, slot):
        return self.hop(dm, dev, self.far(slot), self.frecv(slot))

    def swap(self):
        for dm in (3, 2, 1, 0):
            self.to_partner(dm).start()

    def add(self, dm, *more):
        dst = self.part(self.pos.blk(dm))
        srcs = (dst, self.prx(dm)) + more

        def body(row):
            rows = pl.ds(row, 16)
            total = srcs[0][rows, :].astype(F32)
            for ref in srcs[1:]:
                total = total + ref[rows, :].astype(F32)
            dst[rows, :] = total.astype(BF)

        row_loop(body)

    def step(self, i, q):
        p = self.pos
        if q == 0:
            dm = 4 - i
            self.to_partner(dm).wait_recv()
            self.add(dm)
            self.hop_near(dm, p.away).start()
        elif i < 3:
            dm = 4 - i
            self.to_partner(dm).wait_recv()
            self.hop_near(dm, p.away).wait_recv()
            self.add(dm, self.near(dm - 1))
            self.hop_far(dm, p.away, i - 1).start()
        else:
            self.to_partner(0).wait_recv()
            self.hop_far(0, p.near, 0).wait_recv()
            self.add(0, self.far(0))
            self.hop_far(0, p.near, 0).start()

    def final(self, q, use):
        p = self.pos
        if q == 0:
            self.to_partner(0).wait_recv()
            self.hop_far(0, p.near, 0).wait_recv()
            use((self.part(p.blk(0)), self.prx(0), self.far(0)))
        else:
            self.to_partner(1).wait_recv()
            self.hop_near(1, p.away).wait_recv()
            self.hop_far(1, p.away, 1).wait_recv()
            use((self.part(p.blk(1)), self.prx(1), self.near(0), self.far(1)))

    def drain(self):
        p = self.pos
        for dm in range(4):
            self.to_partner(dm).wait_send()

        def outer():
            for dm in (3, 2, 1):
                self.hop_near(dm, p.away).wait_send()

        def inner():
            for dm in (3, 2, 0):
                self.hop_far(dm, p.away, 0).wait_send()

        p.role(0, outer)
        p.role(1, inner)


def norm_value(wide, gain):
    inv_rms = lax.rsqrt(jnp.mean(wide * wide, axis=-1, keepdims=True) + NORM_EPS)
    return (wide * inv_rms * gain).astype(BF)


RELAY = 256
PER_REQ = OLD // RELAY
N_RELAY = REQ * PER_REQ
RSLOTS = 4
THIRDS = (0, N_RELAY // 3, 2 * N_RELAY // 3, N_RELAY)
KB = 512
FT = 256
N_FULL = FFN // FT
TAIL = FFN - N_FULL * FT
OT = 512
N_OUT = DIM // OT
NT = (((1,), (1,)), ((), ()))
TN = (((0,), (0,)), ((), ()))
SCALE = (HD ** -0.5) * 1.4426950408889634


def layer_kernel(pre_ref, val_ref, x_ref, ga_ref, gm_ref, bq_ref, bk_ref, bv_ref, kc_ref, vc_ref,
                 wq_hbm, wk_hbm, wv_hbm, wo_hbm, wg_hbm, wu_hbm, wd_hbm,
                 out_ref, kn_out, vn_out, kh_out, vh_out,
                 hbuf, wbuf, wgu, wdbuf, part, prx, near, far, mid, ubuf, kv, qbuf, obuf, cosb, sinb,
                 cin, cout, wide, nbuf,
                 wsem, gsem, dsem, isem, csem, ksem, nsem,
                 a1send, a1recv, a2send, a2recv, psend, precv, send, nrecv, frecv):
    pos = Place()

    def span(u):
        return u // PARTS, pl.ds((u % PARTS) * UROWS, UROWS)

    def gather1(r):
        return Gather(pos, lambda t: hbuf.at[r, t], lambda n: a1send.at[r, n], lambda t: a1recv.at[r, t])

    def gather2(u):
        r, rows = span(u)
        return Gather(pos, lambda t: hbuf.at[r, t, rows], lambda n: a2send.at[u, n], lambda t: a2recv.at[u, t])

    def scatter(k, u):
        r, rows = span(u)
        return Scatter(
            pos, lambda t: part.at[r, t, rows], lambda dm: prx.at[r, dm, rows],
            lambda n: near.at[r, n, rows], lambda n: far.at[r, n, rows],
            lambda dm: psend.at[k, u, dm], lambda dm: precv.at[k, u, dm], lambda dm: send.at[k, u, dm],
            lambda n: nrecv.at[k, u, n], lambda n: frecv.at[k, u, n])

    g1 = [gather1(r) for r in range(REQ)]
    g2 = [gather2(u) for u in range(UNITS)]
    rs = [[scatter(k, u) for u in range(UNITS)] for k in range(2)]

    def qkv_load(n):
        return pltpu.make_async_copy((wq_hbm, wk_hbm, wv_hbm)[n % 3], wbuf.at[n % 2], wsem.at[n % 2])

    def wo_load():
        return [pltpu.make_async_copy(wo_hbm.at[pl.ds(w * FT, FT)], wgu.at[0, w], gsem.at[0, w]) for w in range(2)]

    def up_load(n, size=FT):
        rows = pl.ds(pl.multiple_of(n * FT, FT), size)
        return [pltpu.make_async_copy(src.at[rows], wgu.at[n % 2, w, pl.ds(0, size)], gsem.at[n % 2, w])
                for w, src in enumerate((wg_hbm, wu_hbm))]

    def down_load(n, slot):
        cols = pl.ds(pl.multiple_of(n * OT, OT), OT)
        return pltpu.make_async_copy(wd_hbm.at[:, cols], wdbuf.at[slot], dsem.at[slot])

    def relay_in(n, w):
        rows = pl.ds(pl.multiple_of((n % PER_REQ) * RELAY * HEADS, RELAY * HEADS), RELAY * HEADS)
        slot = n % RSLOTS
        return pltpu.make_async_copy((kc_ref, vc_ref)[w].at[n // PER_REQ, rows], cin.at[slot, w], isem.at[slot, w])

    def relay_out(n, w):
        rows = pl.ds(pl.multiple_of((n % PER_REQ) * RELAY, RELAY), RELAY)
        slot = n % RSLOTS
        return pltpu.make_async_copy(cout.at[slot, w], (kh_out, vh_out)[w].at[n // PER_REQ, :, rows], csem.at[slot, w])

    def head_load(r, h, slot):
        return [pltpu.make_async_copy(src.at[r, h], kv.at[slot, w], ksem.at[slot, w])
                for w, src in enumerate((kh_out, vh_out))]

    def new_rows(r, w):
        return pltpu.make_async_copy(nbuf.at[w], (kn_out, vn_out)[w].at[r], nsem.at[w])

    def norm_rows(r):
        gain = ga_ref[...].astype(F32)

        def run(i, carry):
            rows = pl.ds(pl.multiple_of(i * 16, 16), 16)
            hbuf[r, pos.me, rows, :] = norm_value(x_ref[r, rows, :].astype(F32), gain)
            return carry

        lax.fori_loop(0, ROWS // 16, run, 0)

    def pre():
        qkv_load(0).start()
        for n in range(RSLOTS - 1):
            for w in range(2):
                relay_in(n, w).start()
        norm_rows(0)
        entry_barrier(pos)

    def pre2():
        qkv_load(1).start()
        for cp in wo_load():
            cp.start()
        down_load(0, 0).start()
        norm_rows(1)

    def tables():
        half = HD // 2
        lane = lax.broadcasted_iota(jnp.int32, (1, HD), 1)
        freq_id = (lane % half).astype(F32)
        inv_freq = jnp.exp((freq_id * 2.0 / HD) * (-jnp.log(jnp.float32(ROPE_THETA))))
        sign = jnp.where(lane < half, -1.0, 1.0).astype(F32)

        def run(i, carry):
            base = pl.multiple_of(i * 64, 64)
            rows = pl.ds(base, 64)
            row_pos = lax.broadcasted_iota(jnp.int32, (64, 1), 0) + base
            for r in range(REQ):
                angles = (row_pos + pre_ref[r]).astype(F32) * inv_freq
                cosb[r, rows, :] = jnp.cos(angles)
                sinb[r, rows, :] = jnp.sin(angles) * sign
            return carry

        lax.fori_loop(0, CHUNK // 64, run, 0)

    def relay(third):
        def run(n, carry):
            slot = n % RSLOTS
            for w in range(2):
                @pl.when(n + RSLOTS - 1 < N_RELAY)
                def _():
                    relay_in(n + RSLOTS - 1, w).start()

                relay_in(n, w).wait()

                @pl.when(n >= RSLOTS)
                def _():
                    relay_out(n - RSLOTS, w).wait()

                base = w * RELAY * HEADS
                wide[pl.ds(base, RELAY * HEADS), :] = cin[slot, w].astype(F32)
                for h in range(HEADS):
                    cout[slot, w, h] = wide[pl.ds(base + h, RELAY, stride=HEADS), :].astype(BF)
                relay_out(n, w).start()
            return carry

        lax.fori_loop(THIRDS[third], THIRDS[third + 1], run, 0)
        if third == 2:
            for n in range(N_RELAY - RSLOTS, N_RELAY):
                for w in range(2):
                    relay_out(n, w).wait()
            for cp in head_load(0, 0, 0):
                cp.start()

    def qkv(r, i):
        n = r * 3 + i
        qkv_load(n).wait()
        if 1 <= n < 5:
            qkv_load(n + 1).start()
        bias = (bq_ref, bk_ref, bv_ref)[i]

        def run(tile, carry):
            cols = pl.ds(pl.multiple_of(tile * 256, 256), 256)
            acc = jnp.dot(hbuf[r].reshape(CHUNK, DIM), wbuf[n % 2, :, cols], preferred_element_type=F32)
            val = (acc + bias[:, cols].astype(F32)).astype(BF)
            for k in range(2):
                head = val[:, k * HD:(k + 1) * HD]
                if i < 2:
                    wide_head = head.astype(F32)
                    head = (wide_head * cosb[r] + pltpu.roll(wide_head, HD // 2, 1) * sinb[r]).astype(BF)
                qbuf[i, tile * 2 + k] = head
            return carry

        lax.fori_loop(0, 2, run, 0)
        if i > 0:
            w = i - 1
            if r > 0:
                new_rows(r - 1, w).wait()
            for h in range(HEADS):
                wide[pl.ds(h, CHUNK, stride=HEADS), :] = qbuf[i, h].astype(F32)
            nbuf[w] = wide[...].astype(BF)
            new_rows(r, w).start()

    def attend(r, pair):
        prefix = pre_ref[r]
        last = val_ref[r] - 1
        key = lax.broadcasted_iota(jnp.int32, (KB, CHUNK), 0)
        row = lax.broadcasted_iota(jnp.int32, (KB, CHUNK), 1)

        def head(h, carry):
            slot = h % 2
            for cp in head_load(r, h, slot):
                cp.wait()
            if r + 1 < REQ:
                nxt = h + 1
                more = head_load(r + nxt // HEADS, nxt % HEADS, 1 - slot)
                for cp in more:
                    cp.start()
            else:
                @pl.when(h + 1 < HEADS)
                def _():
                    for cp in head_load(r, h + 1, 1 - slot):
                        cp.start()

            q = qbuf[0, h]

            def scores(keys):
                return lax.dot_general(keys, q, NT, preferred_element_type=F32) * SCALE

            s = jnp.where(key <= jnp.minimum(row, last), scores(qbuf[1, h]), -1.0e30)
            m = jnp.max(s, axis=0, keepdims=True)
            probs = jnp.exp2(s - m)
            l = jnp.sum(probs, axis=0, keepdims=True)
            acc = lax.dot_general(qbuf[2, h], probs.astype(BF), TN, preferred_element_type=F32)

            def fold(b, state):
                m, l, acc = state
                rows = pl.ds(pl.multiple_of(b * KB, KB), KB)
                s = jnp.where(key < prefix - b * KB, scores(kv[slot, 0, rows, :]), -1.0e30)
                m_new = jnp.maximum(m, jnp.max(s, axis=0, keepdims=True))
                shrink = jnp.exp2(m - m_new)
                probs = jnp.exp2(s - m_new)
                l = l * shrink + jnp.sum(probs, axis=0, keepdims=True)
                acc = acc * shrink + lax.dot_general(kv[slot, 1, rows, :], probs.astype(BF), TN, preferred_element_type=F32)
                return m_new, l, acc

            m, l, acc = lax.fori_loop(0, OLD // KB, fold, (m, l, acc))
            mixed = (acc / l).T.astype(BF).reshape(RANKS, ROWS, HD)
            obuf[r, :, :, pl.ds(pl.multiple_of(h * HD, HD), HD)] = mixed
            return carry

        lax.fori_loop(2 * pair, 2 * pair + 2, head, 0)

    def store_part(u, cols, value):
        r, rows = span(u)
        part[r, :, rows, cols] = value.astype(BF).reshape(RANKS, UROWS, OT)

    def out_proj(u):
        r, rows = span(u)
        if u % PARTS == 0:
            g1[r].drain()
        if u == 0:
            for cp in wo_load():
                cp.wait()

        def run(n, carry):
            cols = pl.ds(pl.multiple_of(n * OT, OT), OT)
            lhs = obuf[r, :, rows, :].reshape(ULEN, QKV)
            store_part(u, cols, jnp.dot(lhs, wgu[0, :, :, cols].reshape(QKV, OT), preferred_element_type=F32))
            return carry

        lax.fori_loop(0, N_OUT, run, 0)
        if u == UNITS - 1:
            for cp in up_load(0):
                cp.start()

    def act(u, slot, size):
        r, rows = span(u)
        h = hbuf[r, :, rows, :].reshape(ULEN, DIM)
        gate = lax.dot_general(h, wgu[slot, 0, :size], NT, preferred_element_type=F32)
        up = lax.dot_general(h, wgu[slot, 1, :size], NT, preferred_element_type=F32)
        return (gate * (1.0 / (1.0 + jnp.exp(-gate))) * up).astype(BF)

    def mlp_up(u, k):
        def begin(now, after):
            for cp in now:
                cp.wait()
            for cp in after:
                cp.start()

        def run(n, carry):
            begin(up_load(n), up_load(n + 1))
            ubuf[:, pl.ds(pl.multiple_of(n * FT, FT), FT)] = act(u, n % 2, FT)
            return carry

        if k < 2:
            lax.fori_loop(2 * k, 2 * k + 2, run, 0)
        else:
            n = N_FULL - 1
            begin(up_load(n), up_load(N_FULL, TAIL))
            ubuf[:, n * FT:N_FULL * FT] = act(u, n % 2, FT)
            begin(up_load(N_FULL, TAIL), up_load(0) if u + 1 < UNITS else [])
            ubuf[:, N_FULL * FT:] = act(u, N_FULL % 2, TAIL)

    def mlp_down(u, k):
        if k == 0:
            rs[0][u].drain()

        def run(n, carry):
            slot = n % 2
            down_load(n, slot).wait()

            @pl.when(n + 1 < N_OUT)
            def _():
                down_load(n + 1, 1 - slot).start()

            cols = pl.ds(pl.multiple_of(n * OT, OT), OT)
            store_part(u, cols, jnp.dot(ubuf[...], wdbuf[slot], preferred_element_type=F32))
            return carry

        lax.fori_loop(k * N_OUT // 2, (k + 1) * N_OUT // 2, run, 0)
        if k == 1 and u + 1 < UNITS:
            down_load(0, 0).start()

    def summed(refs, rows):
        total = refs[0][rows, :].astype(F32)
        for ref in refs[1:]:
            total = total + ref[rows, :].astype(F32)
        return total.astype(BF).astype(F32)

    def mid_rows(u):
        def use(refs):
            gain = gm_ref[...].astype(F32)
            r = u // PARTS

            def body(row):
                own = pl.ds(row + (u % PARTS) * UROWS, 16)
                x1 = (x_ref[r, own, :].astype(F32) + summed(refs, pl.ds(row, 16))).astype(BF)
                mid[r, own, :] = x1
                hbuf[r, pos.me, own, :] = norm_value(x1.astype(F32), gain)

            row_loop(body)

        return use

    def out_rows(u):
        def use(refs):
            r = u // PARTS

            def body(row):
                own = pl.ds(row + (u % PARTS) * UROWS, 16)
                out_ref[r, own, :] = (mid[r, own, :].astype(F32) + summed(refs, pl.ds(row, 16))).astype(BF)

            row_loop(body)

        return use

    local = {"pre": pre, "pre2": pre2, "rl": relay, "cs": tables, "qkv": qkv, "at": attend,
             "wo": out_proj, "up": mlp_up, "dn": mlp_down}
    remote = {
        "a1": lambda r, i, q: g1[r].step(i, q),
        "a2": lambda u, i, q: g2[u].step(i, q),
        "sw1": lambda u, q: rs[0][u].swap(),
        "sw2": lambda u, q: rs[1][u].swap(),
        "st1": lambda u, i, q: rs[0][u].step(i, q),
        "st2": lambda u, i, q: rs[1][u].step(i, q),
        "fi1": lambda u, q: rs[0][u].final(q, mid_rows(u)),
        "fi2": lambda u, q: rs[1][u].final(q, out_rows(u)),
    }
    pending = []

    def flush():
        for q in (0, 1):
            mine = [op for op in pending if op[-1] == q]
            if mine:
                def run():
                    for op in mine:
                        remote[op[0]](*op[1:])

                pos.role(q, run)
        pending.clear()

    for op in ORDER:
        if op[0] in remote:
            pending.append(op)
        else:
            flush()
            local[op[0]](*op[1:])
    flush()
    for u in range(UNITS):
        g2[u].drain()
        rs[1][u].drain()
    for w in range(2):
        new_rows(REQ - 1, w).wait()


def run_layer(prefix, valid, x_rows, g_attn, g_mlp, b_q, b_k, b_v, k_flat, v_flat, w_q, w_k, w_v, w_o, w_gate_t, w_up_t, w_down):
    vm = pl.BlockSpec(memory_space=pltpu.VMEM)
    sm = pl.BlockSpec(memory_space=pltpu.SMEM)
    anyspace = pl.BlockSpec(memory_space=pl.ANY)
    dma = pltpu.SemaphoreType.DMA
    fresh = jax.ShapeDtypeStruct((REQ, CHUNK * HEADS, HD), BF)
    old = jax.ShapeDtypeStruct((REQ, HEADS, OLD, HD), BF)
    block = (ROWS, DIM)
    return pl.pallas_call(
        layer_kernel,
        out_shape=(jax.ShapeDtypeStruct((REQ,) + block, BF), fresh, fresh, old, old),
        in_specs=[sm, sm] + [vm] * 6 + [anyspace] * 9,
        out_specs=[vm] + [anyspace] * 4,
        scratch_shapes=[
            pltpu.VMEM((REQ, RANKS) + block, BF),
            pltpu.VMEM((2, DIM, QKV), BF),
            pltpu.VMEM((2, 2, FT, DIM), BF),
            pltpu.VMEM((2, FFN, OT), BF),
            pltpu.VMEM((REQ, RANKS) + block, BF),
            pltpu.VMEM((REQ, 4) + block, BF),
            pltpu.VMEM((REQ, 3) + block, BF),
            pltpu.VMEM((REQ, 2) + block, BF),
            pltpu.VMEM((REQ,) + block, BF),
            pltpu.VMEM((ULEN, FFN), BF),
            pltpu.VMEM((2, 2, OLD, HD), BF),
            pltpu.VMEM((3, HEADS, CHUNK, HD), BF),
            pltpu.VMEM((REQ, RANKS, ROWS, QKV), BF),
            pltpu.VMEM((REQ, CHUNK, HD), F32),
            pltpu.VMEM((REQ, CHUNK, HD), F32),
            pltpu.VMEM((RSLOTS, 2, RELAY * HEADS, HD), BF),
            pltpu.VMEM((RSLOTS, 2, HEADS, RELAY, HD), BF),
            pltpu.VMEM((2 * RELAY * HEADS, HD), F32),
            pltpu.VMEM((2, CHUNK * HEADS, HD), BF),
            dma((2,)), dma((2, 2)), dma((2,)), dma((RSLOTS, 2)), dma((RSLOTS, 2)), dma((2, 2)), dma((2,)),
            dma((REQ, 9)), dma((REQ, RANKS)), dma((UNITS, 9)), dma((UNITS, RANKS)),
            dma((2, UNITS, 4)), dma((2, UNITS, 4)), dma((2, UNITS, 4)), dma((2, UNITS, 3)), dma((2, UNITS, 2)),
        ],
        compiler_params=pltpu.CompilerParams(collective_id=0, has_side_effects=True, vmem_limit_bytes=67043328),
        name="layer",
    )(prefix, valid, x_rows, g_attn.reshape(1, DIM), g_mlp.reshape(1, DIM),
      b_q.reshape(1, -1), b_k.reshape(1, -1), b_v.reshape(1, -1),
      k_flat, v_flat, w_q, w_k, w_v, w_o, w_gate_t, w_up_t, w_down)


COPY = 512
N_COPY = 2 * REQ * SLOTS // COPY
CSLOTS = 16


def cache_kernel(pre_ref, val_ref, kc_hbm, vc_hbm, krow_hbm, vrow_hbm, kout_hbm, vout_hbm,
                 cbuf, nbuf, isem, osem, nsem, usem):
    srcs = (kc_hbm, vc_hbm)
    dsts = (kout_hbm, vout_hbm)
    news = (krow_hbm, vrow_hbm)
    per = SLOTS // COPY

    def where(n):
        m = n // 2
        return n % 2, m // per, pl.ds((m % per) * COPY, COPY)

    def take(n):
        w, i, rows = where(n)
        return pltpu.make_async_copy(srcs[w].at[i, rows], cbuf.at[n % CSLOTS], isem.at[n % CSLOTS])

    def put(n):
        w, i, rows = where(n)
        return pltpu.make_async_copy(cbuf.at[n % CSLOTS], dsts[w].at[i, rows], osem.at[n % CSLOTS])

    fresh = [pltpu.make_async_copy(news[w], nbuf.at[w], nsem.at[w]) for w in range(2)]
    for n in range(CSLOTS):
        take(n).start()
    for cp in fresh:
        cp.start()
    lag = CSLOTS // 2
    for n in range(N_COPY):
        take(n).wait()
        put(n).start()
        if n >= lag:
            put(n - lag).wait()
            if n - lag + CSLOTS < N_COPY:
                take(n - lag + CSLOTS).start()
    for n in range(N_COPY - lag, N_COPY):
        put(n).wait()
    for cp in fresh:
        cp.wait()

    def updates(act):
        for i in range(REQ):
            count = val_ref[i]
            for bit in range(10):
                size = 1 << bit
                first = (count >> (bit + 1)) << (bit + 1)

                @pl.when((count >> bit) % 2 == 1)
                def _():
                    for w in range(2):
                        act(pltpu.make_async_copy(
                            nbuf.at[w, i, pl.ds(first, size)],
                            dsts[w].at[i, pl.ds(pre_ref[i] + first, size)],
                            usem.at[w, i, bit]))

    updates(lambda cp: cp.start())
    updates(lambda cp: cp.wait())


def run_cache(prefix, valid, k_cache, v_cache, k_rows, v_rows):
    sm = pl.BlockSpec(memory_space=pltpu.SMEM)
    anyspace = pl.BlockSpec(memory_space=pl.ANY)
    dma = pltpu.SemaphoreType.DMA
    cache = jax.ShapeDtypeStruct((REQ, SLOTS, HEADS, HD), BF)
    return pl.pallas_call(
        cache_kernel,
        out_shape=(cache, cache),
        in_specs=[sm, sm] + [anyspace] * 4,
        out_specs=[anyspace] * 2,
        scratch_shapes=[
            pltpu.VMEM((CSLOTS, COPY, HEADS, HD), BF),
            pltpu.VMEM((2, REQ, CHUNK, HEADS, HD), BF),
            dma((CSLOTS,)), dma((CSLOTS,)), dma((2,)), dma((2, REQ, 10)),
        ],
        compiler_params=pltpu.CompilerParams(vmem_limit_bytes=60 << 20),
        name="cache_write",
    )(prefix, valid, k_cache, v_cache, k_rows, v_rows)


def solution(mesh):
    row_spec = P("dp", "tp", None)
    cache_spec = P("dp", None, "tp", None)
    req_spec = P("dp")
    rep_spec = P(None)
    col_spec = P(None, "tp")
    bias_spec = P("tp")
    down_spec = P("tp", None)

    def layer(x_rows, k_cache, v_cache, prefix, valid, g_attn, w_q, b_q, w_k, b_k, w_v, b_v, w_o, g_mlp, w_gate, w_up, w_down):
        flat = (REQ, SLOTS * HEADS, HD)
        wide = (REQ, CHUNK, HEADS, HD)
        x_out, k_rows, v_rows, _, _ = run_layer(
            prefix, valid, x_rows, g_attn, g_mlp, b_q, b_k, b_v, k_cache.reshape(flat), v_cache.reshape(flat),
            w_q, w_k, w_v, w_o, w_gate.T, w_up.T, w_down)
        k_out, v_out = run_cache(prefix, valid, k_cache, v_cache, k_rows.reshape(wide), v_rows.reshape(wide))
        return x_out, k_out, v_out

    in_specs = (row_spec, cache_spec, cache_spec, req_spec, req_spec, rep_spec, col_spec, bias_spec, col_spec, bias_spec, col_spec, bias_spec, down_spec, rep_spec, col_spec, col_spec, down_spec)
    return jax.shard_map(layer, mesh=mesh, in_specs=in_specs, out_specs=(row_spec, cache_spec, cache_spec), check_vma=False)
```

```python
import jax
import jax.numpy as jnp
from jax import lax
from jax.experimental import pallas as pl
from jax.experimental.pallas import tpu as pltpu
from jax.sharding import PartitionSpec as P

ROPE_THETA = 1.0e6
NORM_EPS = 1.0e-6
MESH = pl.DeviceIdType.MESH
BF = jnp.bfloat16
F32 = jnp.float32

REQ = 2
ROWS = 64
RANKS = 8
CHUNK = ROWS * RANKS
DIM = 4096
HEADS = 4
HD = 128
QKV = HEADS * HD
SLOTS = 4096
OLD = SLOTS - CHUNK
FFN = 1376
PARTS = 2
UNITS = REQ * PARTS
UROWS = ROWS // PARTS
ULEN = CHUNK // PARTS

ORDER = (
    ('pre',), ('a1', 0, 0, 0), ('a1', 0, 0, 1), ('a1', 1, 0, 0), ('a1', 1, 0, 1), ('pre2',), ('a1', 2, 0, 0),
    ('a1', 0, 1, 0), ('a1', 0, 1, 1), ('a1', 0, 2, 1), ('a1', 0, 2, 0), ('rl', 0), ('a1', 3, 0, 0), ('cs',),
    ('rl', 1), ('a1', 1, 1, 1), ('a1', 1, 2, 1), ('rl', 2), ('a1', 0, 3, 1), ('a1', 0, 3, 0), ('a1', 1, 3, 1),
    ('a1', 0, 4, 1), ('a1', 2, 0, 1), ('a1', 1, 1, 0), ('a1', 0, 4, 0), ('a1', 1, 2, 0), ('a1', 1, 4, 1),
    ('a1', 3, 0, 1), ('qkv', 0, 0), ('qkv', 0, 1), ('a1', 1, 3, 0), ('a1', 2, 1, 1), ('qkv', 0, 2), ('a1', 1, 4, 0),
    ('qkv', 1, 0), ('qkv', 1, 1), ('a1', 2, 2, 1), ('qkv', 1, 2), ('a1', 3, 1, 1), ('at', 0, 0), ('at', 0, 1),
    ('wo', 0), ('sw1', 0, 0), ('a1', 2, 1, 0), ('a1', 3, 2, 1), ('wo', 1), ('a1', 3, 1, 0), ('st1', 0, 1, 0),
    ('a1', 2, 3, 1), ('a1', 3, 3, 1), ('st1', 0, 2, 0), ('a1', 2, 2, 0), ('a1', 2, 3, 0), ('a1', 2, 4, 0),
    ('a1', 2, 4, 1), ('qkv', 2, 0), ('sw1', 1, 0), ('qkv', 2, 1), ('a1', 3, 2, 0), ('qkv', 2, 2), ('st1', 1, 1, 0),
    ('a1', 3, 3, 0), ('sw1', 0, 1), ('st1', 1, 2, 0), ('a1', 3, 4, 0), ('a1', 3, 4, 1), ('qkv', 3, 0), ('sw1', 1, 1),
    ('st1', 0, 3, 0), ('st1', 0, 1, 1), ('st1', 1, 3, 0), ('qkv', 3, 1), ('qkv', 3, 2), ('at', 1, 0),
    ('st1', 1, 1, 1), ('st1', 0, 2, 1), ('st1', 0, 3, 1), ('at', 1, 1), ('fi1', 0, 0), ('a2', 0, 0, 0),
    ('st1', 1, 2, 1), ('st1', 1, 3, 1), ('wo', 2), ('fi1', 0, 1), ('wo', 3), ('a2', 0, 0, 1), ('fi1', 1, 1),
    ('sw1', 2, 1), ('a2', 0, 1, 1), ('sw1', 3, 1), ('a2', 1, 0, 1), ('a2', 0, 2, 1), ('fi1', 1, 0), ('sw1', 2, 0),
    ('a2', 1, 0, 0), ('sw1', 3, 0), ('st1', 2, 1, 0), ('st1', 2, 2, 0), ('a2', 1, 1, 1), ('a2', 0, 1, 0),
    ('a2', 0, 3, 1), ('a2', 0, 2, 0), ('st1', 3, 1, 0), ('st1', 3, 2, 0), ('st1', 2, 1, 1), ('a2', 1, 2, 1),
    ('a2', 0, 4, 1), ('a2', 0, 3, 0), ('st1', 2, 3, 0), ('a2', 0, 4, 0), ('up', 0, 0), ('a2', 1, 1, 0), ('up', 0, 1),
    ('st1', 2, 2, 1), ('a2', 1, 2, 0), ('a2', 1, 3, 1), ('up', 0, 2), ('a2', 1, 3, 0), ('st1', 3, 3, 0),
    ('dn', 0, 0), ('a2', 1, 4, 1), ('st1', 3, 1, 1), ('dn', 0, 1), ('sw2', 0, 0), ('st1', 2, 3, 1), ('st1', 3, 2, 1),
    ('fi1', 2, 0), ('fi1', 2, 1), ('a2', 2, 0, 1), ('a2', 1, 4, 0), ('st1', 3, 3, 1), ('a2', 2, 0, 0), ('up', 1, 0),
    ('fi1', 3, 1), ('a2', 2, 1, 1), ('a2', 2, 2, 1), ('st2', 0, 1, 0), ('st2', 0, 2, 0), ('a2', 2, 3, 1),
    ('sw2', 0, 1), ('a2', 3, 0, 1), ('fi1', 3, 0), ('a2', 3, 0, 0), ('up', 1, 1), ('a2', 2, 1, 0), ('up', 1, 2),
    ('dn', 1, 0), ('dn', 1, 1), ('st2', 0, 3, 0), ('sw2', 1, 0), ('a2', 2, 4, 1), ('a2', 3, 1, 1), ('a2', 2, 2, 0),
    ('st2', 1, 1, 0), ('st2', 0, 1, 1), ('a2', 2, 3, 0), ('a2', 2, 4, 0), ('a2', 3, 2, 1), ('st2', 0, 2, 1),
    ('st2', 1, 2, 0), ('sw2', 1, 1), ('up', 2, 0), ('a2', 3, 3, 1), ('up', 2, 1), ('st2', 1, 1, 1), ('up', 2, 2),
    ('a2', 3, 1, 0), ('dn', 2, 0), ('st2', 1, 3, 0), ('dn', 2, 1), ('sw2', 2, 0), ('a2', 3, 2, 0), ('a2', 3, 4, 1),
    ('sw2', 2, 1), ('st2', 2, 1, 0), ('st2', 2, 2, 0), ('a2', 3, 3, 0), ('a2', 3, 4, 0), ('st2', 1, 2, 1),
    ('up', 3, 0), ('up', 3, 1), ('up', 3, 2), ('st2', 2, 1, 1), ('st2', 0, 3, 1), ('dn', 3, 0), ('dn', 3, 1),
    ('st2', 1, 3, 1), ('sw2', 3, 0), ('st2', 2, 2, 1), ('st2', 3, 1, 0), ('st2', 3, 2, 0), ('sw2', 3, 1),
    ('st2', 3, 1, 1), ('st2', 2, 3, 0), ('fi2', 0, 1), ('st2', 3, 3, 0), ('st2', 2, 3, 1), ('fi2', 0, 0),
    ('fi2', 1, 0), ('fi2', 1, 1), ('st2', 3, 2, 1), ('st2', 3, 3, 1), ('fi2', 2, 1), ('fi2', 2, 0), ('fi2', 3, 1),
    ('fi2', 3, 0),
)


class Place:
    def __init__(self):
        t = lax.axis_index("tp")
        self.me = t
        self.c = t % 2
        self.z = t // 2
        self.half = self.z // 2
        self.zm = self.z + self.half * (3 - 2 * self.z)
        self.away = 2 * (self.z + 1 - 2 * self.half) + self.c
        self.near = 2 * (self.z - 1 + 2 * self.half) + self.c
        self.partner = 2 * self.z + 1 - self.c

    def chip(self, dm):
        return dm + self.half * (3 - 2 * dm)

    def blk(self, dm):
        return 2 * self.chip(dm) + self.c

    def other(self, dm):
        return 2 * self.chip(dm) + 1 - self.c

    def role(self, q, fn):
        @pl.when(self.zm == q)
        def _():
            fn()


def entry_barrier(pos):
    bar = pltpu.get_barrier_semaphore()

    def signal(dev):
        pl.semaphore_signal(bar, inc=1, device_id={"tp": dev}, device_id_type=MESH)

    signal(pos.partner)
    signal(pos.away)

    def inner():
        signal(pos.near)
        pl.semaphore_wait(bar, 3)

    pos.role(1, inner)
    pos.role(0, lambda: pl.semaphore_wait(bar, 2))


class Gather:
    def __init__(self, pos, block, send, recv):
        self.pos, self.block, self.send, self.recv = pos, block, send, recv

    def copy(self, t, dev, n):
        ref = self.block(t)
        return pltpu.make_async_remote_copy(
            src_ref=ref, dst_ref=ref, send_sem=self.send(n), recv_sem=self.recv(t),
            device_id={"tp": dev}, device_id_type=MESH)

    def wait_block(self, t):
        self.copy(t, self.pos.partner, 0).wait_recv()

    def step(self, i, q):
        p = self.pos
        if i == 0:
            devs = (p.near, p.away, p.partner) if q else (p.away, p.partner)
            for n, dev in enumerate(devs):
                self.copy(p.me, dev, n).start()
        elif i < 4:
            t = p.blk((0, 2, 3)[i - 1] if q else i)
            self.wait_block(t)
            if q:
                self.copy(t, p.away if i == 1 else p.near, 1 + 2 * i).start()
                self.copy(t, p.partner, 2 + 2 * i).start()
            else:
                self.copy(t, p.partner, 1 + i).start()
        else:
            for dm in range(4):
                self.wait_block(p.other(dm))

    def drain(self):
        p = self.pos

        def wait(count):
            for n in range(count):
                self.copy(p.me, p.partner, n).wait_send()

        p.role(0, lambda: wait(5))
        p.role(1, lambda: wait(9))


def row_loop(body):
    def run(i, carry):
        body(pl.multiple_of(i * 16, 16))
        return carry

    lax.fori_loop(0, UROWS // 16, run, 0)


class Scatter:
    def __init__(self, pos, part, prx, near, far, psend, precv, send, nrecv, frecv):
        self.pos, self.part, self.prx, self.near, self.far = pos, part, prx, near, far
        self.psend, self.precv, self.send, self.nrecv, self.frecv = psend, precv, send, nrecv, frecv

    def to_partner(self, dm):
        p = self.pos
        return pltpu.make_async_remote_copy(
            src_ref=self.part(p.other(dm)), dst_ref=self.prx(dm), send_sem=self.psend(dm),
            recv_sem=self.precv(dm), device_id={"tp": p.partner}, device_id_type=MESH)

    def hop(self, dm, dev, dst, recv):
        return pltpu.make_async_remote_copy(
            src_ref=self.part(self.pos.blk(dm)), dst_ref=dst, send_sem=self.send(dm),
            recv_sem=recv, device_id={"tp": dev}, device_id_type=MESH)

    def hop_near(self, dm, dev):
        return self.hop(dm, dev, self.near(dm - 1), self.nrecv(dm - 1))

    def hop_far(self, dm, dev, slot):
        return self.hop(dm, dev, self.far(slot), self.frecv(slot))

    def swap(self):
        for dm in (3, 2, 1, 0):
            self.to_partner(dm).start()

    def add(self, dm, *more):
        dst = self.part(self.pos.blk(dm))
        srcs = (dst, self.prx(dm)) + more

        def body(row):
            rows = pl.ds(row, 16)
            total = srcs[0][rows, :].astype(F32)
            for ref in srcs[1:]:
                total = total + ref[rows, :].astype(F32)
            dst[rows, :] = total.astype(BF)

        row_loop(body)

    def step(self, i, q):
        p = self.pos
        if q == 0:
            dm = 4 - i
            self.to_partner(dm).wait_recv()
            self.add(dm)
            self.hop_near(dm, p.away).start()
        elif i < 3:
            dm = 4 - i
            self.to_partner(dm).wait_recv()
            self.hop_near(dm, p.away).wait_recv()
            self.add(dm, self.near(dm - 1))
            self.hop_far(dm, p.away, i - 1).start()
        else:
            self.to_partner(0).wait_recv()
            self.hop_far(0, p.near, 0).wait_recv()
            self.add(0, self.far(0))
            self.hop_far(0, p.near, 0).start()

    def final(self, q, use):
        p = self.pos
        if q == 0:
            self.to_partner(0).wait_recv()
            self.hop_far(0, p.near, 0).wait_recv()
            use((self.part(p.blk(0)), self.prx(0), self.far(0)))
        else:
            self.to_partner(1).wait_recv()
            self.hop_near(1, p.away).wait_recv()
            self.hop_far(1, p.away, 1).wait_recv()
            use((self.part(p.blk(1)), self.prx(1), self.near(0), self.far(1)))

    def drain(self):
        p = self.pos
        for dm in range(4):
            self.to_partner(dm).wait_send()

        def outer():
            for dm in (3, 2, 1):
                self.hop_near(dm, p.away).wait_send()

        def inner():
            for dm in (3, 2, 0):
                self.hop_far(dm, p.away, 0).wait_send()

        p.role(0, outer)
        p.role(1, inner)


def norm_value(wide, gain):
    inv_rms = lax.rsqrt(jnp.mean(wide * wide, axis=-1, keepdims=True) + NORM_EPS)
    return (wide * inv_rms * gain).astype(BF)


RELAY = 256
PER_REQ = OLD // RELAY
N_RELAY = REQ * PER_REQ
RSLOTS = 4
THIRDS = (0, N_RELAY // 3, 2 * N_RELAY // 3, N_RELAY)
KB = 512
FT = 256
N_FULL = FFN // FT
TAIL = FFN - N_FULL * FT
OT = 512
N_OUT = DIM // OT
NT = (((1,), (1,)), ((), ()))
TN = (((0,), (0,)), ((), ()))
SCALE = (HD ** -0.5) * 1.4426950408889634


def layer_kernel(pre_ref, val_ref, x_ref, ga_ref, gm_ref, bq_ref, bk_ref, bv_ref, kc_ref, vc_ref,
                 wq_hbm, wk_hbm, wv_hbm, wo_hbm, wg_hbm, wu_hbm, wd_hbm,
                 out_ref, kn_out, vn_out, kh_out, vh_out,
                 hbuf, part, prx, near, far, mid,
                 wsem, osem, msem, isem, csem, ksem, nsem,
                 a1send, a1recv, a2send, a2recv, psend, precv, send, nrecv, frecv):
    pos = Place()

    def span(u):
        return u // PARTS, pl.ds((u % PARTS) * UROWS, UROWS)

    def gather(u, sends, recvs):
        r, rows = span(u)
        return Gather(pos, lambda t: hbuf.at[r, t, rows], lambda n: sends.at[u, n], lambda t: recvs.at[u, t])

    def scatter(k, u):
        r, rows = span(u)
        return Scatter(
            pos, lambda t: part.at[r, t, rows], lambda dm: prx.at[r, dm, rows],
            lambda n: near.at[r, n, rows], lambda n: far.at[r, n, rows],
            lambda dm: psend.at[k, u, dm], lambda dm: precv.at[k, u, dm], lambda dm: send.at[k, u, dm],
            lambda n: nrecv.at[k, u, n], lambda n: frecv.at[k, u, n])

    g1 = [gather(u, a1send, a1recv) for u in range(UNITS)]
    g2 = [gather(u, a2send, a2recv) for u in range(UNITS)]
    rs = [[scatter(k, u) for u in range(UNITS)] for k in range(2)]

    mem = {}

    def qkv_load(n):
        return pltpu.make_async_copy((wq_hbm, wk_hbm, wv_hbm)[n], mem["wbuf"].at[n], wsem.at[n])

    def wo_load():
        return pltpu.make_async_copy(wo_hbm, mem["wo"], osem)

    def mlp_load(w):
        return pltpu.make_async_copy((wg_hbm, wu_hbm, wd_hbm)[w], mem[("wg", "wu", "wd")[w]], msem.at[w])

    def relay_in(n, w):
        rows = pl.ds(pl.multiple_of((n % PER_REQ) * RELAY * HEADS, RELAY * HEADS), RELAY * HEADS)
        slot = n % RSLOTS
        return pltpu.make_async_copy((kc_ref, vc_ref)[w].at[n // PER_REQ, rows], mem["cin"].at[slot, w], isem.at[slot, w])

    def relay_out(n, w):
        rows = pl.ds(pl.multiple_of((n % PER_REQ) * RELAY, RELAY), RELAY)
        slot = n % RSLOTS
        return pltpu.make_async_copy(mem["cout"].at[slot, w], (kh_out, vh_out)[w].at[n // PER_REQ, :, rows], csem.at[slot, w])

    def head_load(r, h, slot):
        return [pltpu.make_async_copy(src.at[r, h], mem["kv"].at[slot, w], ksem.at[slot, w])
                for w, src in enumerate((kh_out, vh_out))]

    def new_rows(r, w):
        return pltpu.make_async_copy(mem["nbuf"].at[w], (kn_out, vn_out)[w].at[r], nsem.at[w])

    def norm_rows(r):
        gain = ga_ref[...].astype(F32).reshape(1, DIM)

        def run(i, carry):
            rows = pl.ds(pl.multiple_of(i * 16, 16), 16)
            hbuf[r, pos.me, rows, :] = norm_value(x_ref[r, rows, :].astype(F32), gain)
            return carry

        lax.fori_loop(0, ROWS // 16, run, 0)

    def pre():
        for n in range(3):
            qkv_load(n).start()
        for n in range(RSLOTS - 1):
            for w in range(2):
                relay_in(n, w).start()
        norm_rows(0)
        entry_barrier(pos)

    def pre2():
        wo_load().start()
        norm_rows(1)

    def tables():
        cosb, sinb = mem["cosb"], mem["sinb"]
        half = HD // 2
        lane = lax.broadcasted_iota(jnp.int32, (1, HD), 1)
        freq_id = (lane % half).astype(F32)
        inv_freq = jnp.exp((freq_id * 2.0 / HD) * (-jnp.log(jnp.float32(ROPE_THETA))))
        sign = jnp.where(lane < half, -1.0, 1.0).astype(F32)

        def run(i, carry):
            row_pos = lax.broadcasted_iota(jnp.int32, (ROWS, 1), 0) + i * ROWS
            for r in range(REQ):
                angles = (row_pos + pre_ref[r]).astype(F32) * inv_freq
                cosb[r, i] = jnp.cos(angles)
                sinb[r, i] = jnp.sin(angles) * sign
            return carry

        lax.fori_loop(0, RANKS, run, 0)

    def relay(third):
        cin, cout, wide = mem["cin"], mem["cout"], mem["wide"]

        def run(n, carry):
            slot = n % RSLOTS
            for w in range(2):
                @pl.when(n + RSLOTS - 1 < N_RELAY)
                def _():
                    relay_in(n + RSLOTS - 1, w).start()

                relay_in(n, w).wait()

                @pl.when(n >= RSLOTS)
                def _():
                    relay_out(n - RSLOTS, w).wait()

                base = w * RELAY * HEADS
                wide[pl.ds(base, RELAY * HEADS), :] = cin[slot, w].astype(F32)
                for h in range(HEADS):
                    cout[slot, w, h] = wide[pl.ds(base + h, RELAY, stride=HEADS), :].astype(BF)
                relay_out(n, w).start()
            return carry

        lax.fori_loop(THIRDS[third], THIRDS[third + 1], run, 0)
        if third == 2:
            for n in range(N_RELAY - RSLOTS, N_RELAY):
                for w in range(2):
                    relay_out(n, w).wait()
            for cp in head_load(0, 0, 0):
                cp.start()

    def qkv(u, i):
        wbuf, qbuf, cosb, sinb, wide, nbuf = (mem[k] for k in ("wbuf", "qbuf", "cosb", "sinb", "wide", "nbuf"))
        r, rows = span(u)
        if u == 0:
            qkv_load(i).wait()
        bias = (bq_ref, bk_ref, bv_ref)[i]

        def run(tile, carry):
            cols = pl.ds(pl.multiple_of(tile * 256, 256), 256)
            lhs = hbuf[r, :, rows, :].reshape(ULEN, DIM)
            acc = jnp.dot(lhs, wbuf[i, :, cols], preferred_element_type=F32)
            val = (acc + bias[cols].astype(F32).reshape(1, 256)).astype(BF)
            for k in range(2):
                head = val[:, k * HD:(k + 1) * HD]
                if i < 2:
                    wide_head = head.astype(F32)
                    cos_t = cosb[r, :, rows, :].reshape(ULEN, HD)
                    sin_t = sinb[r, :, rows, :].reshape(ULEN, HD)
                    head = (wide_head * cos_t + pltpu.roll(wide_head, HD // 2, 1) * sin_t).astype(BF)
                qbuf[i, tile * 2 + k, :, rows, :] = head.reshape(RANKS, UROWS, HD)
            return carry

        lax.fori_loop(0, 2, run, 0)
        if i > 0 and u % PARTS == PARTS - 1:
            w = i - 1
            if r > 0:
                new_rows(r - 1, w).wait()
            for h in range(HEADS):
                wide[pl.ds(h, CHUNK, stride=HEADS), :] = qbuf[i, h].reshape(CHUNK, HD).astype(F32)
            nbuf[w] = wide[...].astype(BF)
            new_rows(r, w).start()

    def attend(r, pair):
        qbuf, obuf, kv = mem["qbuf"], mem["obuf"], mem["kv"]
        prefix = pre_ref[r]
        last = val_ref[r] - 1
        key = lax.broadcasted_iota(jnp.int32, (KB, CHUNK), 0)
        row = lax.broadcasted_iota(jnp.int32, (KB, CHUNK), 1)

        def head(h, carry):
            slot = h % 2
            for cp in head_load(r, h, slot):
                cp.wait()
            if r + 1 < REQ:
                nxt = h + 1
                more = head_load(r + nxt // HEADS, nxt % HEADS, 1 - slot)
                for cp in more:
                    cp.start()
            else:
                @pl.when(h + 1 < HEADS)
                def _():
                    for cp in head_load(r, h + 1, 1 - slot):
                        cp.start()

            q = qbuf[0, h].reshape(CHUNK, HD)

            def scores(keys):
                return lax.dot_general(keys, q, NT, preferred_element_type=F32) * SCALE

            s = jnp.where(key <= jnp.minimum(row, last), scores(qbuf[1, h].reshape(CHUNK, HD)), -1.0e30)
            m = jnp.max(s, axis=0, keepdims=True)
            probs = jnp.exp2(s - m)
            l = jnp.sum(probs, axis=0, keepdims=True)
            acc = lax.dot_general(qbuf[2, h].reshape(CHUNK, HD), probs.astype(BF), TN, preferred_element_type=F32)

            def fold(b, state):
                m, l, acc = state
                rows = pl.ds(pl.multiple_of(b * KB, KB), KB)
                s = jnp.where(key < prefix - b * KB, scores(kv[slot, 0, rows, :]), -1.0e30)
                m_new = jnp.maximum(m, jnp.max(s, axis=0, keepdims=True))
                shrink = jnp.exp2(m - m_new)
                probs = jnp.exp2(s - m_new)
                l = l * shrink + jnp.sum(probs, axis=0, keepdims=True)
                acc = acc * shrink + lax.dot_general(kv[slot, 1, rows, :], probs.astype(BF), TN, preferred_element_type=F32)
                return m_new, l, acc

            m, l, acc = lax.fori_loop(0, OLD // KB, fold, (m, l, acc))
            mixed = (acc / l).T.astype(BF).reshape(RANKS, ROWS, HD)
            obuf[r, :, :, pl.ds(pl.multiple_of(h * HD, HD), HD)] = mixed
            return carry

        lax.fori_loop(2 * pair, 2 * pair + 2, head, 0)

    def store_part(u, cols, value):
        r, rows = span(u)
        part[r, :, rows, cols] = value.astype(BF).reshape(RANKS, UROWS, OT)

    def out_proj(u):
        r, rows = span(u)
        if u % PARTS == 0:
            for part_id in range(PARTS):
                g1[u + part_id].drain()
        if u == 0:
            wo_load().wait()
        obuf, wo = mem["obuf"], mem["wo"]

        def run(n, carry):
            cols = pl.ds(pl.multiple_of(n * OT, OT), OT)
            lhs = obuf[r, :, rows, :].reshape(ULEN, QKV)
            store_part(u, cols, jnp.dot(lhs, wo[:, cols], preferred_element_type=F32))
            return carry

        lax.fori_loop(0, N_OUT, run, 0)

    def act(u, tile, size):
        r, rows = span(u)
        h = hbuf[r, :, rows, :].reshape(ULEN, DIM)
        gate = lax.dot_general(h, mem["wg"][tile, :], NT, preferred_element_type=F32)
        up = lax.dot_general(h, mem["wu"][tile, :], NT, preferred_element_type=F32)
        mem["ubuf"][:, tile] = (gate * (1.0 / (1.0 + jnp.exp(-gate))) * up).astype(BF)

    def mlp_up(u, k):
        if u == 0 and k == 0:
            mlp_load(0).wait()
            mlp_load(1).wait()

        def run(n, carry):
            act(u, pl.ds(pl.multiple_of(n * FT, FT), FT), FT)
            return carry

        if k < 2:
            lax.fori_loop(2 * k, 2 * k + 2, run, 0)
        else:
            act(u, slice((N_FULL - 1) * FT, N_FULL * FT), FT)
            act(u, slice(N_FULL * FT, FFN), TAIL)

    def mlp_down(u, k):
        if k == 0:
            rs[0][u].drain()
        if u == 0 and k == 0:
            mlp_load(2).wait()

        def run(n, carry):
            cols = pl.ds(pl.multiple_of(n * OT, OT), OT)
            store_part(u, cols, jnp.dot(mem["ubuf"][...], mem["wd"][:, cols], preferred_element_type=F32))
            return carry

        lax.fori_loop(k * N_OUT // 2, (k + 1) * N_OUT // 2, run, 0)

    def summed(refs, rows):
        total = refs[0][rows, :].astype(F32)
        for ref in refs[1:]:
            total = total + ref[rows, :].astype(F32)
        return total.astype(BF).astype(F32)

    def mid_rows(u):
        def use(refs):
            gain = gm_ref[...].astype(F32).reshape(1, DIM)
            r = u // PARTS

            def body(row):
                own = pl.ds(row + (u % PARTS) * UROWS, 16)
                x1 = (x_ref[r, own, :].astype(F32) + summed(refs, pl.ds(row, 16))).astype(BF)
                mid[r, own, :] = x1
                hbuf[r, pos.me, own, :] = norm_value(x1.astype(F32), gain)

            row_loop(body)

        return use

    def out_rows(u):
        def use(refs):
            r = u // PARTS

            def body(row):
                own = pl.ds(row + (u % PARTS) * UROWS, 16)
                out_ref[r, own, :] = (mid[r, own, :].astype(F32) + summed(refs, pl.ds(row, 16))).astype(BF)

            row_loop(body)

        return use

    local = {"pre": pre, "pre2": pre2, "rl": relay, "cs": tables, "qkv": qkv, "at": attend,
             "wo": out_proj, "up": mlp_up, "dn": mlp_down}
    remote = {
        "a1": lambda u, i, q: g1[u].step(i, q),
        "a2": lambda u, i, q: g2[u].step(i, q),
        "sw1": lambda u, q: rs[0][u].swap(),
        "sw2": lambda u, q: rs[1][u].swap(),
        "st1": lambda u, i, q: rs[0][u].step(i, q),
        "st2": lambda u, i, q: rs[1][u].step(i, q),
        "fi1": lambda u, q: rs[0][u].final(q, mid_rows(u)),
        "fi2": lambda u, q: rs[1][u].final(q, out_rows(u)),
    }
    pending = []

    def flush():
        for q in (0, 1):
            mine = [op for op in pending if op[-1] == q]
            if mine:
                def run():
                    for op in mine:
                        remote[op[0]](*op[1:])

                pos.role(q, run)
        pending.clear()

    def play(ops):
        for op in ops:
            if op[0] in remote:
                pending.append(op)
            else:
                flush()
                local[op[0]](*op[1:])
        flush()

    cut = ORDER.index(("wo", UNITS - 1)) + 1

    def attention_phase(**refs):
        mem.update(refs)
        play(ORDER[:cut])
        for w in range(2):
            new_rows(REQ - 1, w).wait()

    def mlp_phase(**refs):
        mem.update(refs)
        for w in range(3):
            mlp_load(w).start()
        play(ORDER[cut:])

    pl.run_scoped(
        attention_phase,
        wbuf=pltpu.VMEM((3, DIM, QKV), BF),
        wo=pltpu.VMEM((QKV, DIM), BF),
        kv=pltpu.VMEM((2, 2, OLD, HD), BF),
        qbuf=pltpu.VMEM((3, HEADS, RANKS, ROWS, HD), BF),
        obuf=pltpu.VMEM((REQ, RANKS, ROWS, QKV), BF),
        cosb=pltpu.VMEM((REQ, RANKS, ROWS, HD), F32),
        sinb=pltpu.VMEM((REQ, RANKS, ROWS, HD), F32),
        cin=pltpu.VMEM((RSLOTS, 2, RELAY * HEADS, HD), BF),
        cout=pltpu.VMEM((RSLOTS, 2, HEADS, RELAY, HD), BF),
        wide=pltpu.VMEM((2 * RELAY * HEADS, HD), F32),
        nbuf=pltpu.VMEM((2, CHUNK * HEADS, HD), BF),
    )
    pl.run_scoped(
        mlp_phase,
        wg=pltpu.VMEM((FFN, DIM), BF),
        wu=pltpu.VMEM((FFN, DIM), BF),
        wd=pltpu.VMEM((FFN, DIM), BF),
        ubuf=pltpu.VMEM((ULEN, FFN), BF),
    )
    for u in range(UNITS):
        g2[u].drain()
        rs[1][u].drain()


def run_layer(prefix, valid, x_rows, g_attn, g_mlp, b_q, b_k, b_v, k_flat, v_flat, w_q, w_k, w_v, w_o, w_gate_t, w_up_t, w_down):
    vm = pl.BlockSpec(memory_space=pltpu.VMEM)
    sm = pl.BlockSpec(memory_space=pltpu.SMEM)
    anyspace = pl.BlockSpec(memory_space=pl.ANY)
    dma = pltpu.SemaphoreType.DMA
    fresh = jax.ShapeDtypeStruct((REQ, CHUNK * HEADS, HD), BF)
    old = jax.ShapeDtypeStruct((REQ, HEADS, OLD, HD), BF)
    block = (ROWS, DIM)
    return pl.pallas_call(
        layer_kernel,
        out_shape=(jax.ShapeDtypeStruct((REQ,) + block, BF), fresh, fresh, old, old),
        in_specs=[sm, sm] + [vm] * 6 + [anyspace] * 9,
        out_specs=[vm] + [anyspace] * 4,
        scratch_shapes=[
            pltpu.VMEM((REQ, RANKS) + block, BF),
            pltpu.VMEM((REQ, RANKS) + block, BF),
            pltpu.VMEM((REQ, 4) + block, BF),
            pltpu.VMEM((REQ, 3) + block, BF),
            pltpu.VMEM((REQ, 2) + block, BF),
            pltpu.VMEM((REQ,) + block, BF),
            dma((3,)), dma, dma((3,)), dma((RSLOTS, 2)), dma((RSLOTS, 2)), dma((2, 2)), dma((2,)),
            dma((UNITS, 9)), dma((UNITS, RANKS)), dma((UNITS, 9)), dma((UNITS, RANKS)),
            dma((2, UNITS, 4)), dma((2, UNITS, 4)), dma((2, UNITS, 4)), dma((2, UNITS, 3)), dma((2, UNITS, 2)),
        ],
        compiler_params=pltpu.CompilerParams(collective_id=0, has_side_effects=True, vmem_limit_bytes=67043328),
        name="layer",
    )(prefix, valid, x_rows, g_attn, g_mlp, b_q, b_k, b_v, k_flat, v_flat, w_q, w_k, w_v, w_o, w_gate_t, w_up_t, w_down)


COPY = 512
N_COPY = 2 * REQ * SLOTS // COPY
CSLOTS = 16


def cache_kernel(pre_ref, val_ref, kc_hbm, vc_hbm, krow_hbm, vrow_hbm, kout_hbm, vout_hbm,
                 cbuf, nbuf, isem, osem, nsem, usem):
    srcs = (kc_hbm, vc_hbm)
    dsts = (kout_hbm, vout_hbm)
    news = (krow_hbm, vrow_hbm)
    per = SLOTS // COPY

    def where(n):
        m = n // 2
        return n % 2, m // per, pl.ds((m % per) * COPY, COPY)

    def take(n):
        w, i, rows = where(n)
        return pltpu.make_async_copy(srcs[w].at[i, rows], cbuf.at[n % CSLOTS], isem.at[n % CSLOTS])

    def put(n):
        w, i, rows = where(n)
        return pltpu.make_async_copy(cbuf.at[n % CSLOTS], dsts[w].at[i, rows], osem.at[n % CSLOTS])

    fresh = [pltpu.make_async_copy(news[w], nbuf.at[w], nsem.at[w]) for w in range(2)]
    for n in range(CSLOTS):
        take(n).start()
    for cp in fresh:
        cp.start()
    lag = CSLOTS // 2
    for n in range(N_COPY):
        take(n).wait()
        put(n).start()
        if n >= lag:
            put(n - lag).wait()
            if n - lag + CSLOTS < N_COPY:
                take(n - lag + CSLOTS).start()
    for n in range(N_COPY - lag, N_COPY):
        put(n).wait()
    for cp in fresh:
        cp.wait()

    def updates(act):
        for i in range(REQ):
            count = val_ref[i]
            for bit in range(10):
                size = 1 << bit
                first = (count >> (bit + 1)) << (bit + 1)

                @pl.when((count >> bit) % 2 == 1)
                def _():
                    for w in range(2):
                        act(pltpu.make_async_copy(
                            nbuf.at[w, i, pl.ds(first, size)],
                            dsts[w].at[i, pl.ds(pre_ref[i] + first, size)],
                            usem.at[w, i, bit]))

    updates(lambda cp: cp.start())
    updates(lambda cp: cp.wait())


def run_cache(prefix, valid, k_cache, v_cache, k_rows, v_rows):
    sm = pl.BlockSpec(memory_space=pltpu.SMEM)
    anyspace = pl.BlockSpec(memory_space=pl.ANY)
    dma = pltpu.SemaphoreType.DMA
    cache = jax.ShapeDtypeStruct((REQ, SLOTS, HEADS, HD), BF)
    return pl.pallas_call(
        cache_kernel,
        out_shape=(cache, cache),
        in_specs=[sm, sm] + [anyspace] * 4,
        out_specs=[anyspace] * 2,
        scratch_shapes=[
            pltpu.VMEM((CSLOTS, COPY, HEADS, HD), BF),
            pltpu.VMEM((2, REQ, CHUNK, HEADS, HD), BF),
            dma((CSLOTS,)), dma((CSLOTS,)), dma((2,)), dma((2, REQ, 10)),
        ],
        compiler_params=pltpu.CompilerParams(vmem_limit_bytes=60 << 20),
        name="cache_write",
    )(prefix, valid, k_cache, v_cache, k_rows, v_rows)


def solution(mesh):
    row_spec = P("dp", "tp", None)
    cache_spec = P("dp", None, "tp", None)
    req_spec = P("dp")
    rep_spec = P(None)
    col_spec = P(None, "tp")
    bias_spec = P("tp")
    down_spec = P("tp", None)

    def layer(x_rows, k_cache, v_cache, prefix, valid, g_attn, w_q, b_q, w_k, b_k, w_v, b_v, w_o, g_mlp, w_gate, w_up, w_down):
        flat = (REQ, SLOTS * HEADS, HD)
        wide = (REQ, CHUNK, HEADS, HD)
        x_out, k_rows, v_rows, _, _ = run_layer(
            prefix, valid, x_rows, g_attn, g_mlp, b_q, b_k, b_v, k_cache.reshape(flat), v_cache.reshape(flat),
            w_q, w_k, w_v, w_o, w_gate.T, w_up.T, w_down)
        k_out, v_out = run_cache(prefix, valid, k_cache, v_cache, k_rows.reshape(wide), v_rows.reshape(wide))
        return x_out, k_out, v_out

    in_specs = (row_spec, cache_spec, cache_spec, req_spec, req_spec, rep_spec, col_spec, bias_spec, col_spec, bias_spec, col_spec, bias_spec, down_spec, rep_spec, col_spec, col_spec, down_spec)
    return jax.shard_map(layer, mesh=mesh, in_specs=in_specs, out_specs=(row_spec, cache_spec, cache_spec), check_vma=False)
```

```python
import jax
import jax.numpy as jnp
from jax import lax
from jax.experimental import pallas as pl
from jax.experimental.pallas import tpu as pltpu
from jax.sharding import PartitionSpec as P

ROPE_THETA = 1.0e6
NORM_EPS = 1.0e-6
MESH = pl.DeviceIdType.MESH
BF = jnp.bfloat16
F32 = jnp.float32

REQ = 2
ROWS = 64
RANKS = 8
CHUNK = ROWS * RANKS
DIM = 4096
HEADS = 4
HD = 128
QKV = HEADS * HD
SLOTS = 4096
OLD = SLOTS - CHUNK
FFN = 1376
PARTS = 2
UNITS = REQ * PARTS
UROWS = ROWS // PARTS
ULEN = CHUNK // PARTS

ORDER = (
    ('pre',), ('a1', 0, 0, 1), ('a1', 0, 0, 0), ('a1', 1, 0, 1), ('a1', 0, 1, 1), ('a1', 1, 0, 0), ('a1', 0, 2, 1),
    ('pre2',), ('a1', 1, 1, 1), ('a1', 1, 2, 1), ('rl', 0), ('a1', 2, 0, 0), ('a1', 0, 3, 1), ('a1', 1, 3, 1),
    ('a1', 0, 1, 0), ('a1', 1, 1, 0), ('a1', 3, 0, 0), ('rl', 1), ('a1', 2, 0, 1), ('a1', 0, 2, 0), ('a1', 3, 0, 1),
    ('rl', 2), ('a1', 0, 4, 1), ('a1', 1, 4, 1), ('cs',), ('a1', 0, 3, 0), ('a1', 0, 4, 0), ('qkv', 0, 0),
    ('qkv', 0, 1), ('a1', 1, 2, 0), ('a1', 1, 3, 0), ('a1', 2, 1, 1), ('qkv', 0, 2), ('a1', 1, 4, 0), ('qkv', 1, 0),
    ('qkv', 1, 1), ('a1', 2, 2, 1), ('a1', 3, 1, 1), ('qkv', 1, 2), ('at', 0, 0), ('a1', 2, 3, 1), ('a1', 3, 2, 1),
    ('at', 0, 1), ('a1', 2, 1, 0), ('wo', 0), ('sw1', 0, 0), ('a1', 2, 2, 0), ('a1', 3, 3, 1), ('wo', 1),
    ('st1', 0, 1, 0), ('sw1', 1, 0), ('st1', 0, 2, 0), ('st1', 1, 1, 0), ('a1', 2, 3, 0), ('a1', 3, 1, 0),
    ('st1', 1, 2, 0), ('a1', 2, 4, 0), ('a1', 2, 4, 1), ('sw1', 0, 1), ('st1', 0, 3, 0), ('qkv', 2, 0),
    ('qkv', 2, 1), ('qkv', 2, 2), ('a1', 3, 2, 0), ('a1', 3, 3, 0), ('sw1', 1, 1), ('a1', 3, 4, 0), ('a1', 3, 4, 1),
    ('qkv', 3, 0), ('qkv', 3, 1), ('qkv', 3, 2), ('st1', 0, 1, 1), ('at', 1, 0), ('st1', 1, 3, 0), ('st1', 0, 2, 1),
    ('st1', 0, 3, 1), ('st1', 1, 1, 1), ('at', 1, 1), ('st1', 1, 2, 1), ('fi1', 0, 0), ('wo', 2), ('a2', 0, 0, 0),
    ('sw1', 2, 0), ('fi1', 0, 1), ('a2', 0, 0, 1), ('sw1', 2, 1), ('st1', 1, 3, 1), ('wo', 3), ('fi1', 1, 1),
    ('sw1', 3, 0), ('st1', 2, 1, 0), ('a2', 1, 0, 1), ('sw1', 3, 1), ('a2', 0, 1, 1), ('st1', 2, 2, 0),
    ('st1', 3, 1, 0), ('a2', 0, 2, 1), ('fi1', 1, 0), ('a2', 1, 0, 0), ('st1', 2, 1, 1), ('a2', 0, 3, 1),
    ('a2', 0, 1, 0), ('st1', 2, 2, 1), ('st1', 3, 2, 0), ('st1', 3, 1, 1), ('st1', 2, 3, 0), ('a2', 0, 2, 0),
    ('st1', 2, 3, 1), ('a2', 1, 1, 1), ('a2', 0, 4, 1), ('a2', 1, 2, 1), ('fi1', 2, 0), ('a2', 2, 0, 0),
    ('a2', 0, 3, 0), ('a2', 1, 1, 0), ('a2', 0, 4, 0), ('st1', 3, 3, 0), ('up', 0, 0), ('up', 0, 1),
    ('st1', 3, 2, 1), ('st1', 3, 3, 1), ('up', 0, 2), ('a2', 1, 2, 0), ('a2', 1, 3, 1), ('fi1', 2, 1),
    ('a2', 2, 0, 1), ('fi1', 3, 0), ('a2', 3, 0, 0), ('dn', 0, 0), ('a2', 2, 1, 1), ('dn', 0, 1), ('sw2', 0, 0),
    ('a2', 1, 3, 0), ('a2', 1, 4, 1), ('st2', 0, 1, 0), ('sw2', 0, 1), ('a2', 1, 4, 0), ('up', 1, 0),
    ('a2', 2, 2, 1), ('fi1', 3, 1), ('up', 1, 1), ('st2', 0, 2, 0), ('a2', 2, 1, 0), ('up', 1, 2), ('a2', 2, 3, 1),
    ('a2', 3, 0, 1), ('dn', 1, 0), ('dn', 1, 1), ('sw2', 1, 1), ('st2', 0, 3, 0), ('a2', 3, 1, 1), ('a2', 3, 2, 1),
    ('a2', 2, 4, 1), ('sw2', 1, 0), ('a2', 2, 2, 0), ('a2', 2, 3, 0), ('st2', 1, 1, 0), ('st2', 0, 1, 1),
    ('a2', 2, 4, 0), ('up', 2, 0), ('a2', 3, 3, 1), ('st2', 0, 2, 1), ('st2', 1, 2, 0), ('up', 2, 1), ('up', 2, 2),
    ('a2', 3, 1, 0), ('dn', 2, 0), ('dn', 2, 1), ('a2', 3, 4, 1), ('st2', 0, 3, 1), ('st2', 1, 3, 0),
    ('a2', 3, 2, 0), ('sw2', 2, 0), ('st2', 1, 1, 1), ('st2', 2, 1, 0), ('a2', 3, 3, 0), ('st2', 2, 2, 0),
    ('a2', 3, 4, 0), ('sw2', 2, 1), ('up', 3, 0), ('up', 3, 1), ('up', 3, 2), ('fi2', 0, 1), ('st2', 1, 2, 1),
    ('dn', 3, 0), ('dn', 3, 1), ('sw2', 3, 0), ('st2', 2, 1, 1), ('sw2', 3, 1), ('st2', 2, 2, 1), ('st2', 3, 1, 0),
    ('st2', 3, 2, 0), ('st2', 1, 3, 1), ('st2', 3, 1, 1), ('st2', 2, 3, 1), ('fi2', 0, 0), ('st2', 2, 3, 0),
    ('fi2', 1, 1), ('st2', 3, 2, 1), ('fi2', 1, 0), ('st2', 3, 3, 0), ('st2', 3, 3, 1), ('fi2', 2, 1), ('fi2', 2, 0),
    ('fi2', 3, 1), ('fi2', 3, 0),
)


class Place:
    def __init__(self):
        t = lax.axis_index("tp")
        self.me = t
        self.c = t % 2
        self.z = t // 2
        self.half = self.z // 2
        self.zm = self.z + self.half * (3 - 2 * self.z)
        self.away = 2 * (self.z + 1 - 2 * self.half) + self.c
        self.near = 2 * (self.z - 1 + 2 * self.half) + self.c
        self.partner = 2 * self.z + 1 - self.c

    def chip(self, dm):
        return dm + self.half * (3 - 2 * dm)

    def blk(self, dm):
        return 2 * self.chip(dm) + self.c

    def other(self, dm):
        return 2 * self.chip(dm) + 1 - self.c

    def role(self, q, fn):
        @pl.when(self.zm == q)
        def _():
            fn()


def entry_barrier(pos):
    bar = pltpu.get_barrier_semaphore()

    def signal(dev):
        pl.semaphore_signal(bar, inc=1, device_id={"tp": dev}, device_id_type=MESH)

    signal(pos.partner)
    signal(pos.away)

    def inner():
        signal(pos.near)
        pl.semaphore_wait(bar, 3)

    pos.role(1, inner)
    pos.role(0, lambda: pl.semaphore_wait(bar, 2))


class Gather:
    def __init__(self, pos, block, send, recv):
        self.pos, self.block, self.send, self.recv = pos, block, send, recv

    def copy(self, t, dev, n):
        ref = self.block(t)
        return pltpu.make_async_remote_copy(
            src_ref=ref, dst_ref=ref, send_sem=self.send(n), recv_sem=self.recv(t),
            device_id={"tp": dev}, device_id_type=MESH)

    def wait_block(self, t):
        self.copy(t, self.pos.partner, 0).wait_recv()

    def step(self, i, q):
        p = self.pos
        if i == 0:
            devs = (p.near, p.away, p.partner) if q else (p.away, p.partner)
            for n, dev in enumerate(devs):
                self.copy(p.me, dev, n).start()
        elif i < 4:
            t = p.blk((0, 2, 3)[i - 1] if q else i)
            self.wait_block(t)
            if q:
                self.copy(t, p.away if i == 1 else p.near, 1 + 2 * i).start()
                self.copy(t, p.partner, 2 + 2 * i).start()
            else:
                self.copy(t, p.partner, 1 + i).start()
        else:
            for dm in range(4):
                self.wait_block(p.other(dm))

    def drain(self):
        p = self.pos

        def wait(count):
            for n in range(count):
                self.copy(p.me, p.partner, n).wait_send()

        p.role(0, lambda: wait(5))
        p.role(1, lambda: wait(9))


def row_loop(body):
    def run(i, carry):
        body(pl.multiple_of(i * 16, 16))
        return carry

    lax.fori_loop(0, UROWS // 16, run, 0)


class Scatter:
    def __init__(self, pos, part, prx, near, far, psend, precv, send, nrecv, frecv):
        self.pos, self.part, self.prx, self.near, self.far = pos, part, prx, near, far
        self.psend, self.precv, self.send, self.nrecv, self.frecv = psend, precv, send, nrecv, frecv

    def to_partner(self, dm):
        p = self.pos
        return pltpu.make_async_remote_copy(
            src_ref=self.part(p.other(dm)), dst_ref=self.prx(dm), send_sem=self.psend(dm),
            recv_sem=self.precv(dm), device_id={"tp": p.partner}, device_id_type=MESH)

    def hop(self, dm, dev, dst, recv):
        return pltpu.make_async_remote_copy(
            src_ref=self.part(self.pos.blk(dm)), dst_ref=dst, send_sem=self.send(dm),
            recv_sem=recv, device_id={"tp": dev}, device_id_type=MESH)

    def hop_near(self, dm, dev):
        return self.hop(dm, dev, self.near(dm - 1), self.nrecv(dm - 1))

    def hop_far(self, dm, dev, slot):
        return self.hop(dm, dev, self.far(slot), self.frecv(slot))

    def swap(self):
        for dm in (3, 2, 1, 0):
            self.to_partner(dm).start()

    def add(self, dm, *more):
        dst = self.part(self.pos.blk(dm))
        srcs = (dst, self.prx(dm)) + more

        def body(row):
            rows = pl.ds(row, 16)
            total = srcs[0][rows, :].astype(F32)
            for ref in srcs[1:]:
                total = total + ref[rows, :].astype(F32)
            dst[rows, :] = total.astype(BF)

        row_loop(body)

    def step(self, i, q):
        p = self.pos
        if q == 0:
            dm = 4 - i
            self.to_partner(dm).wait_recv()
            self.add(dm)
            self.hop_near(dm, p.away).start()
        elif i < 3:
            dm = 4 - i
            self.to_partner(dm).wait_recv()
            self.hop_near(dm, p.away).wait_recv()
            self.add(dm, self.near(dm - 1))
            self.hop_far(dm, p.away, i - 1).start()
        else:
            self.to_partner(0).wait_recv()
            self.hop_far(0, p.near, 0).wait_recv()
            self.add(0, self.far(0))
            self.hop_far(0, p.near, 0).start()

    def final(self, q, use):
        p = self.pos
        if q == 0:
            self.to_partner(0).wait_recv()
            self.hop_far(0, p.near, 0).wait_recv()
            use((self.part(p.blk(0)), self.prx(0), self.far(0)))
        else:
            self.to_partner(1).wait_recv()
            self.hop_near(1, p.away).wait_recv()
            self.hop_far(1, p.away, 1).wait_recv()
            use((self.part(p.blk(1)), self.prx(1), self.near(0), self.far(1)))

    def drain(self):
        p = self.pos
        for dm in range(4):
            self.to_partner(dm).wait_send()

        def outer():
            for dm in (3, 2, 1):
                self.hop_near(dm, p.away).wait_send()

        def inner():
            for dm in (3, 2, 0):
                self.hop_far(dm, p.away, 0).wait_send()

        p.role(0, outer)
        p.role(1, inner)


def norm_value(wide, gain):
    inv_rms = lax.rsqrt(jnp.mean(wide * wide, axis=-1, keepdims=True) + NORM_EPS)
    return (wide * inv_rms * gain).astype(BF)


RELAY = 256
PER_REQ = OLD // RELAY
N_RELAY = REQ * PER_REQ
RSLOTS = 4
THIRDS = (0, N_RELAY // 3, 2 * N_RELAY // 3, N_RELAY)
KB = 512
FT = 256
N_FULL = FFN // FT
TAIL = FFN - N_FULL * FT
OT = 512
N_OUT = DIM // OT
NT = (((1,), (1,)), ((), ()))
TN = (((0,), (0,)), ((), ()))
SCALE = (HD ** -0.5) * 1.4426950408889634


def layer_kernel(pre_ref, val_ref, x_ref, ga_ref, gm_ref, bq_ref, bk_ref, bv_ref, kc_ref, vc_ref,
                 wq_hbm, wk_hbm, wv_hbm, wo_hbm, wg_hbm, wu_hbm, wd_hbm,
                 out_ref, kn_out, vn_out, kh_out, vh_out,
                 hbuf, part, prx, near, far, mid,
                 wsem, osem, msem, isem, csem, ksem, nsem,
                 a1send, a1recv, a2send, a2recv, psend, precv, send, nrecv, frecv):
    pos = Place()

    def span(u):
        return u // PARTS, pl.ds((u % PARTS) * UROWS, UROWS)

    def gather(u, sends, recvs):
        r, rows = span(u)
        return Gather(pos, lambda t: hbuf.at[r, t, rows], lambda n: sends.at[u, n], lambda t: recvs.at[u, t])

    def scatter(k, u):
        r, rows = span(u)
        return Scatter(
            pos, lambda t: part.at[r, t, rows], lambda dm: prx.at[r, dm, rows],
            lambda n: near.at[r, n, rows], lambda n: far.at[r, n, rows],
            lambda dm: psend.at[k, u, dm], lambda dm: precv.at[k, u, dm], lambda dm: send.at[k, u, dm],
            lambda n: nrecv.at[k, u, n], lambda n: frecv.at[k, u, n])

    g1 = [gather(u, a1send, a1recv) for u in range(UNITS)]
    g2 = [gather(u, a2send, a2recv) for u in range(UNITS)]
    rs = [[scatter(k, u) for u in range(UNITS)] for k in range(2)]

    mem = {}

    def qkv_load(n):
        return pltpu.make_async_copy((wq_hbm, wk_hbm, wv_hbm)[n], mem["wbuf"].at[n], wsem.at[n])

    def wo_load():
        return pltpu.make_async_copy(wo_hbm, mem["wo"], osem)

    def mlp_load(w):
        return pltpu.make_async_copy((wg_hbm, wu_hbm, wd_hbm)[w], mem[("wg", "wu", "wd")[w]], msem.at[w])

    def relay_in(n, w):
        rows = pl.ds(pl.multiple_of((n % PER_REQ) * RELAY * HEADS, RELAY * HEADS), RELAY * HEADS)
        slot = n % RSLOTS
        return pltpu.make_async_copy((kc_ref, vc_ref)[w].at[n // PER_REQ, rows], mem["cin"].at[slot, w], isem.at[slot, w])

    def relay_out(n, w):
        rows = pl.ds(pl.multiple_of((n % PER_REQ) * RELAY, RELAY), RELAY)
        slot = n % RSLOTS
        return pltpu.make_async_copy(mem["cout"].at[slot, w], (kh_out, vh_out)[w].at[n // PER_REQ, :, rows], csem.at[slot, w])

    def head_load(r, h, slot):
        return [pltpu.make_async_copy(src.at[r, h], mem["kv"].at[slot, w], ksem.at[slot, w])
                for w, src in enumerate((kh_out, vh_out))]

    def new_rows(r, w):
        return pltpu.make_async_copy(mem["nbuf"].at[w], (kn_out, vn_out)[w].at[r], nsem.at[w])

    def norm_rows(r):
        gain = ga_ref[...].astype(F32).reshape(1, DIM)

        def run(i, carry):
            rows = pl.ds(pl.multiple_of(i * 16, 16), 16)
            hbuf[r, pos.me, rows, :] = norm_value(x_ref[r, rows, :].astype(F32), gain)
            return carry

        lax.fori_loop(0, ROWS // 16, run, 0)

    def pre():
        for n in range(3):
            qkv_load(n).start()
        for n in range(RSLOTS - 1):
            for w in range(2):
                relay_in(n, w).start()
        norm_rows(0)
        entry_barrier(pos)

    def pre2():
        wo_load().start()
        norm_rows(1)

    def tables():
        cosb, sinb = mem["cosb"], mem["sinb"]
        half = HD // 2
        lane = lax.broadcasted_iota(jnp.int32, (1, HD), 1)
        freq_id = (lane % half).astype(F32)
        inv_freq = jnp.exp((freq_id * 2.0 / HD) * (-jnp.log(jnp.float32(ROPE_THETA))))
        sign = jnp.where(lane < half, -1.0, 1.0).astype(F32)

        def run(i, carry):
            row_pos = lax.broadcasted_iota(jnp.int32, (ROWS, 1), 0) + i * ROWS
            for r in range(REQ):
                angles = (row_pos + pre_ref[r]).astype(F32) * inv_freq
                cosb[r, i] = jnp.cos(angles)
                sinb[r, i] = jnp.sin(angles) * sign
            return carry

        lax.fori_loop(0, RANKS, run, 0)

    def relay(third):
        cin, cout, wide = mem["cin"], mem["cout"], mem["wide"]

        def run(n, carry):
            slot = n % RSLOTS
            for w in range(2):
                @pl.when(n + RSLOTS - 1 < N_RELAY)
                def _():
                    relay_in(n + RSLOTS - 1, w).start()

                relay_in(n, w).wait()

                @pl.when(n >= RSLOTS)
                def _():
                    relay_out(n - RSLOTS, w).wait()

                base = w * RELAY * HEADS
                wide[pl.ds(base, RELAY * HEADS), :] = cin[slot, w].astype(F32)
                for h in range(HEADS):
                    cout[slot, w, h] = wide[pl.ds(base + h, RELAY, stride=HEADS), :].astype(BF)
                relay_out(n, w).start()
            return carry

        lax.fori_loop(THIRDS[third], THIRDS[third + 1], run, 0)
        if third == 2:
            for n in range(N_RELAY - RSLOTS, N_RELAY):
                for w in range(2):
                    relay_out(n, w).wait()
            for cp in head_load(0, 0, 0):
                cp.start()

    def qkv(u, i):
        wbuf, qbuf, cosb, sinb, wide, nbuf = (mem[k] for k in ("wbuf", "qbuf", "cosb", "sinb", "wide", "nbuf"))
        r, rows = span(u)
        if u == 0:
            qkv_load(i).wait()
        bias = (bq_ref, bk_ref, bv_ref)[i]

        def run(tile, carry):
            cols = pl.ds(pl.multiple_of(tile * 256, 256), 256)
            lhs = hbuf[r, :, rows, :].reshape(ULEN, DIM)
            acc = jnp.dot(lhs, wbuf[i, :, cols], preferred_element_type=F32)
            val = (acc + bias[cols].astype(F32).reshape(1, 256)).astype(BF)
            for k in range(2):
                head = val[:, k * HD:(k + 1) * HD]
                if i < 2:
                    wide_head = head.astype(F32)
                    cos_t = cosb[r, :, rows, :].reshape(ULEN, HD)
                    sin_t = sinb[r, :, rows, :].reshape(ULEN, HD)
                    head = (wide_head * cos_t + pltpu.roll(wide_head, HD // 2, 1) * sin_t).astype(BF)
                qbuf[i, tile * 2 + k, :, rows, :] = head.reshape(RANKS, UROWS, HD)
            return carry

        lax.fori_loop(0, 2, run, 0)
        if i > 0 and u % PARTS == PARTS - 1:
            w = i - 1
            if r > 0:
                new_rows(r - 1, w).wait()
            for h in range(HEADS):
                wide[pl.ds(h, CHUNK, stride=HEADS), :] = qbuf[i, h].reshape(CHUNK, HD).astype(F32)
            nbuf[w] = wide[...].astype(BF)
            new_rows(r, w).start()

    def attend(r, pair):
        qbuf, obuf, kv = mem["qbuf"], mem["obuf"], mem["kv"]
        prefix = pre_ref[r]
        last = val_ref[r] - 1
        key = lax.broadcasted_iota(jnp.int32, (KB, CHUNK), 0)
        row = lax.broadcasted_iota(jnp.int32, (KB, CHUNK), 1)

        def head(h, carry):
            slot = h % 2
            for cp in head_load(r, h, slot):
                cp.wait()
            if r + 1 < REQ:
                nxt = h + 1
                more = head_load(r + nxt // HEADS, nxt % HEADS, 1 - slot)
                for cp in more:
                    cp.start()
            else:
                @pl.when(h + 1 < HEADS)
                def _():
                    for cp in head_load(r, h + 1, 1 - slot):
                        cp.start()

            q = qbuf[0, h].reshape(CHUNK, HD)

            def scores(keys):
                return lax.dot_general(keys, q, NT, preferred_element_type=F32) * SCALE

            s = jnp.where(key <= jnp.minimum(row, last), scores(qbuf[1, h].reshape(CHUNK, HD)), -1.0e30)
            m = jnp.max(s, axis=0, keepdims=True)
            probs = jnp.exp2(s - m)
            l = jnp.sum(probs, axis=0, keepdims=True)
            acc = lax.dot_general(qbuf[2, h].reshape(CHUNK, HD), probs.astype(BF), TN, preferred_element_type=F32)

            def fold(b, state):
                m, l, acc = state
                rows = pl.ds(pl.multiple_of(b * KB, KB), KB)
                s = jnp.where(key < prefix - b * KB, scores(kv[slot, 0, rows, :]), -1.0e30)
                m_new = jnp.maximum(m, jnp.max(s, axis=0, keepdims=True))
                shrink = jnp.exp2(m - m_new)
                probs = jnp.exp2(s - m_new)
                l = l * shrink + jnp.sum(probs, axis=0, keepdims=True)
                acc = acc * shrink + lax.dot_general(kv[slot, 1, rows, :], probs.astype(BF), TN, preferred_element_type=F32)
                return m_new, l, acc

            m, l, acc = lax.fori_loop(0, OLD // KB, fold, (m, l, acc))
            mixed = (acc / l).T.astype(BF).reshape(RANKS, ROWS, HD)
            obuf[r, :, :, pl.ds(pl.multiple_of(h * HD, HD), HD)] = mixed
            return carry

        lax.fori_loop(2 * pair, 2 * pair + 2, head, 0)

    def store_part(u, cols, value):
        r, rows = span(u)
        part[r, :, rows, cols] = value.astype(BF).reshape(RANKS, UROWS, OT)

    def out_proj(u):
        r, rows = span(u)
        if u % PARTS == 0:
            for part_id in range(PARTS):
                g1[u + part_id].drain()
        if u == 0:
            wo_load().wait()
        obuf, wo = mem["obuf"], mem["wo"]

        def run(n, carry):
            cols = pl.ds(pl.multiple_of(n * OT, OT), OT)
            lhs = obuf[r, :, rows, :].reshape(ULEN, QKV)
            store_part(u, cols, jnp.dot(lhs, wo[:, cols], preferred_element_type=F32))
            return carry

        lax.fori_loop(0, N_OUT, run, 0)

    def act(u, tile, size):
        r, rows = span(u)
        h = hbuf[r, :, rows, :].reshape(ULEN, DIM)
        gate = lax.dot_general(h, mem["wg"][tile, :], NT, preferred_element_type=F32)
        up = lax.dot_general(h, mem["wu"][tile, :], NT, preferred_element_type=F32)
        mem["ubuf"][:, tile] = (gate * (1.0 / (1.0 + jnp.exp(-gate))) * up).astype(BF)

    def mlp_up(u, k):
        if u == 0 and k == 0:
            mlp_load(0).wait()
            mlp_load(1).wait()

        def run(n, carry):
            act(u, pl.ds(pl.multiple_of(n * FT, FT), FT), FT)
            return carry

        if k < 2:
            lax.fori_loop(2 * k, 2 * k + 2, run, 0)
        else:
            act(u, slice((N_FULL - 1) * FT, N_FULL * FT), FT)
            act(u, slice(N_FULL * FT, FFN), TAIL)

    def mlp_down(u, k):
        if k == 0:
            rs[0][u].drain()
        if u == 0 and k == 0:
            mlp_load(2).wait()

        def run(n, carry):
            cols = pl.ds(pl.multiple_of(n * OT, OT), OT)
            store_part(u, cols, jnp.dot(mem["ubuf"][...], mem["wd"][:, cols], preferred_element_type=F32))
            return carry

        lax.fori_loop(k * N_OUT // 2, (k + 1) * N_OUT // 2, run, 0)

    def summed(refs, rows):
        total = refs[0][rows, :].astype(F32)
        for ref in refs[1:]:
            total = total + ref[rows, :].astype(F32)
        return total.astype(BF).astype(F32)

    def mid_rows(u):
        def use(refs):
            gain = gm_ref[...].astype(F32).reshape(1, DIM)
            r = u // PARTS

            def body(row):
                own = pl.ds(row + (u % PARTS) * UROWS, 16)
                x1 = (x_ref[r, own, :].astype(F32) + summed(refs, pl.ds(row, 16))).astype(BF)
                mid[r, own, :] = x1
                hbuf[r, pos.me, own, :] = norm_value(x1.astype(F32), gain)

            row_loop(body)

        return use

    def out_rows(u):
        def use(refs):
            r = u // PARTS

            def body(row):
                own = pl.ds(row + (u % PARTS) * UROWS, 16)
                out_ref[r, own, :] = (mid[r, own, :].astype(F32) + summed(refs, pl.ds(row, 16))).astype(BF)

            row_loop(body)

        return use

    local = {"pre": pre, "pre2": pre2, "rl": relay, "cs": tables, "qkv": qkv, "at": attend,
             "wo": out_proj, "up": mlp_up, "dn": mlp_down}
    remote = {
        "a1": lambda u, i, q: g1[u].step(i, q),
        "a2": lambda u, i, q: g2[u].step(i, q),
        "sw1": lambda u, q: rs[0][u].swap(),
        "sw2": lambda u, q: rs[1][u].swap(),
        "st1": lambda u, i, q: rs[0][u].step(i, q),
        "st2": lambda u, i, q: rs[1][u].step(i, q),
        "fi1": lambda u, q: rs[0][u].final(q, mid_rows(u)),
        "fi2": lambda u, q: rs[1][u].final(q, out_rows(u)),
    }
    pending = []

    def flush():
        for q in (0, 1):
            mine = [op for op in pending if op[-1] == q]
            if mine:
                def run():
                    for op in mine:
                        remote[op[0]](*op[1:])

                pos.role(q, run)
        pending.clear()

    def play(ops):
        for op in ops:
            if op[0] in remote:
                pending.append(op)
            else:
                flush()
                local[op[0]](*op[1:])
        flush()

    cut = ORDER.index(("wo", UNITS - 1)) + 1

    def attention_phase(**refs):
        mem.update(refs)
        play(ORDER[:cut])
        for w in range(2):
            new_rows(REQ - 1, w).wait()

    def mlp_phase(**refs):
        mem.update(refs)
        for w in range(3):
            mlp_load(w).start()
        play(ORDER[cut:])

    pl.run_scoped(
        attention_phase,
        wbuf=pltpu.VMEM((3, DIM, QKV), BF),
        wo=pltpu.VMEM((QKV, DIM), BF),
        kv=pltpu.VMEM((2, 2, OLD, HD), BF),
        qbuf=pltpu.VMEM((3, HEADS, RANKS, ROWS, HD), BF),
        obuf=pltpu.VMEM((REQ, RANKS, ROWS, QKV), BF),
        cosb=pltpu.VMEM((REQ, RANKS, ROWS, HD), F32),
        sinb=pltpu.VMEM((REQ, RANKS, ROWS, HD), F32),
        cin=pltpu.VMEM((RSLOTS, 2, RELAY * HEADS, HD), BF),
        cout=pltpu.VMEM((RSLOTS, 2, HEADS, RELAY, HD), BF),
        wide=pltpu.VMEM((2 * RELAY * HEADS, HD), F32),
        nbuf=pltpu.VMEM((2, CHUNK * HEADS, HD), BF),
    )
    pl.run_scoped(
        mlp_phase,
        wg=pltpu.VMEM((FFN, DIM), BF),
        wu=pltpu.VMEM((FFN, DIM), BF),
        wd=pltpu.VMEM((FFN, DIM), BF),
        ubuf=pltpu.VMEM((ULEN, FFN), BF),
    )
    for u in range(UNITS):
        g2[u].drain()
        rs[1][u].drain()


def run_layer(prefix, valid, x_rows, g_attn, g_mlp, b_q, b_k, b_v, k_flat, v_flat, w_q, w_k, w_v, w_o, w_gate_t, w_up_t, w_down):
    vm = pl.BlockSpec(memory_space=pltpu.VMEM)
    sm = pl.BlockSpec(memory_space=pltpu.SMEM)
    anyspace = pl.BlockSpec(memory_space=pl.ANY)
    dma = pltpu.SemaphoreType.DMA
    fresh = jax.ShapeDtypeStruct((REQ, CHUNK * HEADS, HD), BF)
    old = jax.ShapeDtypeStruct((REQ, HEADS, OLD, HD), BF)
    block = (ROWS, DIM)
    return pl.pallas_call(
        layer_kernel,
        out_shape=(jax.ShapeDtypeStruct((REQ,) + block, BF), fresh, fresh, old, old),
        in_specs=[sm, sm] + [vm] * 6 + [anyspace] * 9,
        out_specs=[vm] + [anyspace] * 4,
        scratch_shapes=[
            pltpu.VMEM((REQ, RANKS) + block, BF),
            pltpu.VMEM((REQ, RANKS) + block, BF),
            pltpu.VMEM((REQ, 4) + block, BF),
            pltpu.VMEM((REQ, 3) + block, BF),
            pltpu.VMEM((REQ, 2) + block, BF),
            pltpu.VMEM((REQ,) + block, BF),
            dma((3,)), dma, dma((3,)), dma((RSLOTS, 2)), dma((RSLOTS, 2)), dma((2, 2)), dma((2,)),
            dma((UNITS, 9)), dma((UNITS, RANKS)), dma((UNITS, 9)), dma((UNITS, RANKS)),
            dma((2, UNITS, 4)), dma((2, UNITS, 4)), dma((2, UNITS, 4)), dma((2, UNITS, 3)), dma((2, UNITS, 2)),
        ],
        compiler_params=pltpu.CompilerParams(collective_id=0, has_side_effects=True, vmem_limit_bytes=67043328),
        name="layer",
    )(prefix, valid, x_rows, g_attn, g_mlp, b_q, b_k, b_v, k_flat, v_flat, w_q, w_k, w_v, w_o, w_gate_t, w_up_t, w_down)


COPY = 1024
N_COPY = SLOTS // COPY


def cache_kernel(pre_ref, val_ref, kc_hbm, vc_hbm, krow_hbm, vrow_hbm, kout_hbm, vout_hbm,
                 cbuf, nbuf, isem, osem, nsem, usem):
    srcs = (kc_hbm, vc_hbm)
    dsts = (kout_hbm, vout_hbm)
    news = (krow_hbm, vrow_hbm)
    groups = [(w, i) for w in range(2) for i in range(REQ)]

    def takes(w, i):
        return [pltpu.make_async_copy(srcs[w].at[i, pl.ds(n * COPY, COPY)], cbuf.at[w, i, pl.ds(n * COPY, COPY)], isem.at[w, i, n])
                for n in range(N_COPY)]

    def puts(w, i):
        return [pltpu.make_async_copy(cbuf.at[w, i, pl.ds(n * COPY, COPY)], dsts[w].at[i, pl.ds(n * COPY, COPY)], osem.at[w, i, n])
                for n in range(N_COPY)]

    def updates(w, i, act):
        count = val_ref[i]
        for bit in range(10):
            size = 1 << bit
            first = (count >> (bit + 1)) << (bit + 1)

            @pl.when((count >> bit) % 2 == 1)
            def _():
                act(pltpu.make_async_copy(
                    nbuf.at[w, i, pl.ds(first, size)],
                    cbuf.at[w, i, pl.ds(pre_ref[i] + first, size)],
                    usem.at[w, i, bit]))

    fresh = [pltpu.make_async_copy(news[w], nbuf.at[w], nsem.at[w]) for w in range(2)]
    for w, i in groups:
        for cp in takes(w, i):
            cp.start()
        if i == 0:
            fresh[w].start()
    for w, i in groups:
        for cp in takes(w, i):
            cp.wait()
        if i == 0:
            fresh[w].wait()
        updates(w, i, lambda cp: cp.start())
        updates(w, i, lambda cp: cp.wait())
        for cp in puts(w, i):
            cp.start()
    for w, i in groups:
        for cp in puts(w, i):
            cp.wait()


def run_cache(prefix, valid, k_cache, v_cache, k_rows, v_rows):
    sm = pl.BlockSpec(memory_space=pltpu.SMEM)
    anyspace = pl.BlockSpec(memory_space=pl.ANY)
    dma = pltpu.SemaphoreType.DMA
    cache = jax.ShapeDtypeStruct((REQ, SLOTS, HEADS, HD), BF)
    return pl.pallas_call(
        cache_kernel,
        out_shape=(cache, cache),
        in_specs=[sm, sm] + [anyspace] * 4,
        out_specs=[anyspace] * 2,
        scratch_shapes=[
            pltpu.VMEM((2, REQ, SLOTS, HEADS, HD), BF),
            pltpu.VMEM((2, REQ, CHUNK, HEADS, HD), BF),
            dma((2, REQ, N_COPY)), dma((2, REQ, N_COPY)), dma((2,)), dma((2, REQ, 10)),
        ],
        compiler_params=pltpu.CompilerParams(vmem_limit_bytes=60 << 20),
        name="cache_write",
    )(prefix, valid, k_cache, v_cache, k_rows, v_rows)


def solution(mesh):
    row_spec = P("dp", "tp", None)
    cache_spec = P("dp", None, "tp", None)
    req_spec = P("dp")
    rep_spec = P(None)
    col_spec = P(None, "tp")
    bias_spec = P("tp")
    down_spec = P("tp", None)

    def layer(x_rows, k_cache, v_cache, prefix, valid, g_attn, w_q, b_q, w_k, b_k, w_v, b_v, w_o, g_mlp, w_gate, w_up, w_down):
        flat = (REQ, SLOTS * HEADS, HD)
        wide = (REQ, CHUNK, HEADS, HD)
        x_out, k_rows, v_rows, _, _ = run_layer(
            prefix, valid, x_rows, g_attn, g_mlp, b_q, b_k, b_v, k_cache.reshape(flat), v_cache.reshape(flat),
            w_q, w_k, w_v, w_o, w_gate.T, w_up.T, w_down)
        k_out, v_out = run_cache(prefix, valid, k_cache, v_cache, k_rows.reshape(wide), v_rows.reshape(wide))
        return x_out, k_out, v_out

    in_specs = (row_spec, cache_spec, cache_spec, req_spec, req_spec, rep_spec, col_spec, bias_spec, col_spec, bias_spec, col_spec, bias_spec, down_spec, rep_spec, col_spec, col_spec, down_spec)
    return jax.shard_map(layer, mesh=mesh, in_specs=in_specs, out_specs=(row_spec, cache_spec, cache_spec), check_vma=False)
```

```python
import jax
import jax.numpy as jnp
from jax import lax
from jax.experimental import pallas as pl
from jax.experimental.pallas import tpu as pltpu
from jax.sharding import PartitionSpec as P

ROPE_THETA = 1.0e6
NORM_EPS = 1.0e-6
MESH = pl.DeviceIdType.MESH
BF = jnp.bfloat16
F32 = jnp.float32

REQ = 2
ROWS = 64
RANKS = 8
CHUNK = ROWS * RANKS
DIM = 4096
HEADS = 4
HD = 128
QKV = HEADS * HD
SLOTS = 4096
OLD = SLOTS - CHUNK
FFN = 1376
PARTS = 2
UNITS = REQ * PARTS
UROWS = ROWS // PARTS
ULEN = CHUNK // PARTS

ORDER = (
    ('pre',), ('a1', 0, 0, 0), ('a1', 0, 0, 1), ('a1', 1, 0, 0), ('a1', 1, 0, 1), ('pre2',), ('a1', 2, 0, 0),
    ('a1', 0, 1, 0), ('a1', 0, 1, 1), ('a1', 0, 2, 1), ('a1', 0, 2, 0), ('rl', 0), ('a1', 3, 0, 0), ('cs',),
    ('rl', 1), ('a1', 1, 1, 1), ('a1', 1, 2, 1), ('rl', 2), ('a1', 0, 3, 1), ('a1', 0, 3, 0), ('a1', 1, 3, 1),
    ('a1', 0, 4, 1), ('a1', 2, 0, 1), ('a1', 1, 1, 0), ('a1', 0, 4, 0), ('a1', 1, 2, 0), ('a1', 1, 4, 1),
    ('a1', 3, 0, 1), ('qkv', 0, 0), ('qkv', 0, 1), ('a1', 1, 3, 0), ('a1', 2, 1, 1), ('qkv', 0, 2), ('a1', 1, 4, 0),
    ('qkv', 1, 0), ('qkv', 1, 1), ('a1', 2, 2, 1), ('qkv', 1, 2), ('a1', 3, 1, 1), ('at', 0, 0), ('at', 0, 1),
    ('wo', 0), ('sw1', 0, 0), ('a1', 2, 1, 0), ('a1', 3, 2, 1), ('wo', 1), ('a1', 3, 1, 0), ('st1', 0, 1, 0),
    ('a1', 2, 3, 1), ('a1', 3, 3, 1), ('st1', 0, 2, 0), ('a1', 2, 2, 0), ('a1', 2, 3, 0), ('a1', 2, 4, 0),
    ('a1', 2, 4, 1), ('qkv', 2, 0), ('sw1', 1, 0), ('qkv', 2, 1), ('a1', 3, 2, 0), ('qkv', 2, 2), ('st1', 1, 1, 0),
    ('a1', 3, 3, 0), ('sw1', 0, 1), ('st1', 1, 2, 0), ('a1', 3, 4, 0), ('a1', 3, 4, 1), ('qkv', 3, 0), ('sw1', 1, 1),
    ('st1', 0, 3, 0), ('st1', 0, 1, 1), ('st1', 1, 3, 0), ('qkv', 3, 1), ('qkv', 3, 2), ('at', 1, 0),
    ('st1', 1, 1, 1), ('st1', 0, 2, 1), ('st1', 0, 3, 1), ('at', 1, 1), ('fi1', 0, 0), ('a2', 0, 0, 0),
    ('st1', 1, 2, 1), ('st1', 1, 3, 1), ('wo', 2), ('fi1', 0, 1), ('wo', 3), ('a2', 0, 0, 1), ('fi1', 1, 1),
    ('sw1', 2, 1), ('a2', 0, 1, 1), ('sw1', 3, 1), ('a2', 1, 0, 1), ('a2', 0, 2, 1), ('fi1', 1, 0), ('sw1', 2, 0),
    ('a2', 1, 0, 0), ('sw1', 3, 0), ('st1', 2, 1, 0), ('st1', 2, 2, 0), ('a2', 1, 1, 1), ('a2', 0, 1, 0),
    ('a2', 0, 3, 1), ('a2', 0, 2, 0), ('st1', 3, 1, 0), ('st1', 3, 2, 0), ('st1', 2, 1, 1), ('a2', 1, 2, 1),
    ('a2', 0, 4, 1), ('a2', 0, 3, 0), ('st1', 2, 3, 0), ('a2', 0, 4, 0), ('up', 0, 0), ('a2', 1, 1, 0), ('up', 0, 1),
    ('st1', 2, 2, 1), ('a2', 1, 2, 0), ('a2', 1, 3, 1), ('up', 0, 2), ('a2', 1, 3, 0), ('st1', 3, 3, 0),
    ('dn', 0, 0), ('a2', 1, 4, 1), ('st1', 3, 1, 1), ('dn', 0, 1), ('sw2', 0, 0), ('st1', 2, 3, 1), ('st1', 3, 2, 1),
    ('fi1', 2, 0), ('fi1', 2, 1), ('a2', 2, 0, 1), ('a2', 1, 4, 0), ('st1', 3, 3, 1), ('a2', 2, 0, 0), ('up', 1, 0),
    ('fi1', 3, 1), ('a2', 2, 1, 1), ('a2', 2, 2, 1), ('st2', 0, 1, 0), ('st2', 0, 2, 0), ('a2', 2, 3, 1),
    ('sw2', 0, 1), ('a2', 3, 0, 1), ('fi1', 3, 0), ('a2', 3, 0, 0), ('up', 1, 1), ('a2', 2, 1, 0), ('up', 1, 2),
    ('dn', 1, 0), ('dn', 1, 1), ('st2', 0, 3, 0), ('sw2', 1, 0), ('a2', 2, 4, 1), ('a2', 3, 1, 1), ('a2', 2, 2, 0),
    ('st2', 1, 1, 0), ('st2', 0, 1, 1), ('a2', 2, 3, 0), ('a2', 2, 4, 0), ('a2', 3, 2, 1), ('st2', 0, 2, 1),
    ('st2', 1, 2, 0), ('sw2', 1, 1), ('up', 2, 0), ('a2', 3, 3, 1), ('up', 2, 1), ('st2', 1, 1, 1), ('up', 2, 2),
    ('a2', 3, 1, 0), ('dn', 2, 0), ('st2', 1, 3, 0), ('dn', 2, 1), ('sw2', 2, 0), ('a2', 3, 2, 0), ('a2', 3, 4, 1),
    ('sw2', 2, 1), ('st2', 2, 1, 0), ('st2', 2, 2, 0), ('a2', 3, 3, 0), ('a2', 3, 4, 0), ('st2', 1, 2, 1),
    ('up', 3, 0), ('up', 3, 1), ('up', 3, 2), ('st2', 2, 1, 1), ('st2', 0, 3, 1), ('dn', 3, 0), ('dn', 3, 1),
    ('st2', 1, 3, 1), ('sw2', 3, 0), ('st2', 2, 2, 1), ('st2', 3, 1, 0), ('st2', 3, 2, 0), ('sw2', 3, 1),
    ('st2', 3, 1, 1), ('st2', 2, 3, 0), ('fi2', 0, 1), ('st2', 3, 3, 0), ('st2', 2, 3, 1), ('fi2', 0, 0),
    ('fi2', 1, 0), ('fi2', 1, 1), ('st2', 3, 2, 1), ('st2', 3, 3, 1), ('fi2', 2, 1), ('fi2', 2, 0), ('fi2', 3, 1),
    ('fi2', 3, 0),
)


class Place:
    def __init__(self):
        t = lax.axis_index("tp")
        self.me = t
        self.c = t % 2
        self.z = t // 2
        self.half = self.z // 2
        self.zm = self.z + self.half * (3 - 2 * self.z)
        self.away = 2 * (self.z + 1 - 2 * self.half) + self.c
        self.near = 2 * (self.z - 1 + 2 * self.half) + self.c
        self.partner = 2 * self.z + 1 - self.c

    def chip(self, dm):
        return dm + self.half * (3 - 2 * dm)

    def blk(self, dm):
        return 2 * self.chip(dm) + self.c

    def other(self, dm):
        return 2 * self.chip(dm) + 1 - self.c

    def role(self, q, fn):
        @pl.when(self.zm == q)
        def _():
            fn()


def entry_barrier(pos):
    bar = pltpu.get_barrier_semaphore()

    def signal(dev):
        pl.semaphore_signal(bar, inc=1, device_id={"tp": dev}, device_id_type=MESH)

    signal(pos.partner)
    signal(pos.away)

    def inner():
        signal(pos.near)
        pl.semaphore_wait(bar, 3)

    pos.role(1, inner)
    pos.role(0, lambda: pl.semaphore_wait(bar, 2))


class Gather:
    def __init__(self, pos, block, send, recv):
        self.pos, self.block, self.send, self.recv = pos, block, send, recv

    def copy(self, t, dev, n):
        ref = self.block(t)
        return pltpu.make_async_remote_copy(
            src_ref=ref, dst_ref=ref, send_sem=self.send(n), recv_sem=self.recv(t),
            device_id={"tp": dev}, device_id_type=MESH)

    def wait_block(self, t):
        self.copy(t, self.pos.partner, 0).wait_recv()

    def step(self, i, q):
        p = self.pos
        if i == 0:
            devs = (p.near, p.away, p.partner) if q else (p.away, p.partner)
            for n, dev in enumerate(devs):
                self.copy(p.me, dev, n).start()
        elif i < 4:
            t = p.blk((0, 2, 3)[i - 1] if q else i)
            self.wait_block(t)
            if q:
                self.copy(t, p.away if i == 1 else p.near, 1 + 2 * i).start()
                self.copy(t, p.partner, 2 + 2 * i).start()
            else:
                self.copy(t, p.partner, 1 + i).start()
        else:
            for dm in range(4):
                self.wait_block(p.other(dm))

    def drain(self):
        p = self.pos

        def wait(count):
            for n in range(count):
                self.copy(p.me, p.partner, n).wait_send()

        p.role(0, lambda: wait(5))
        p.role(1, lambda: wait(9))


def row_loop(body):
    def run(i, carry):
        body(pl.multiple_of(i * 16, 16))
        return carry

    lax.fori_loop(0, UROWS // 16, run, 0)


class Scatter:
    def __init__(self, pos, part, prx, near, far, psend, precv, send, nrecv, frecv):
        self.pos, self.part, self.prx, self.near, self.far = pos, part, prx, near, far
        self.psend, self.precv, self.send, self.nrecv, self.frecv = psend, precv, send, nrecv, frecv

    def to_partner(self, dm):
        p = self.pos
        return pltpu.make_async_remote_copy(
            src_ref=self.part(p.other(dm)), dst_ref=self.prx(dm), send_sem=self.psend(dm),
            recv_sem=self.precv(dm), device_id={"tp": p.partner}, device_id_type=MESH)

    def hop(self, dm, dev, dst, recv):
        return pltpu.make_async_remote_copy(
            src_ref=self.part(self.pos.blk(dm)), dst_ref=dst, send_sem=self.send(dm),
            recv_sem=recv, device_id={"tp": dev}, device_id_type=MESH)

    def hop_near(self, dm, dev):
        return self.hop(dm, dev, self.near(dm - 1), self.nrecv(dm - 1))

    def hop_far(self, dm, dev, slot):
        return self.hop(dm, dev, self.far(slot), self.frecv(slot))

    def swap(self):
        for dm in (3, 2, 1, 0):
            self.to_partner(dm).start()

    def add(self, dm, *more):
        dst = self.part(self.pos.blk(dm))
        srcs = (dst, self.prx(dm)) + more

        def body(row):
            rows = pl.ds(row, 16)
            total = srcs[0][rows, :].astype(F32)
            for ref in srcs[1:]:
                total = total + ref[rows, :].astype(F32)
            dst[rows, :] = total.astype(BF)

        row_loop(body)

    def step(self, i, q):
        p = self.pos
        if q == 0:
            dm = 4 - i
            self.to_partner(dm).wait_recv()
            self.add(dm)
            self.hop_near(dm, p.away).start()
        elif i < 3:
            dm = 4 - i
            self.to_partner(dm).wait_recv()
            self.hop_near(dm, p.away).wait_recv()
            self.add(dm, self.near(dm - 1))
            self.hop_far(dm, p.away, i - 1).start()
        else:
            self.to_partner(0).wait_recv()
            self.hop_far(0, p.near, 0).wait_recv()
            self.add(0, self.far(0))
            self.hop_far(0, p.near, 0).start()

    def final(self, q, use):
        p = self.pos
        if q == 0:
            self.to_partner(0).wait_recv()
            self.hop_far(0, p.near, 0).wait_recv()
            use((self.part(p.blk(0)), self.prx(0), self.far(0)))
        else:
            self.to_partner(1).wait_recv()
            self.hop_near(1, p.away).wait_recv()
            self.hop_far(1, p.away, 1).wait_recv()
            use((self.part(p.blk(1)), self.prx(1), self.near(0), self.far(1)))

    def drain(self):
        p = self.pos
        for dm in range(4):
            self.to_partner(dm).wait_send()

        def outer():
            for dm in (3, 2, 1):
                self.hop_near(dm, p.away).wait_send()

        def inner():
            for dm in (3, 2, 0):
                self.hop_far(dm, p.away, 0).wait_send()

        p.role(0, outer)
        p.role(1, inner)


def norm_value(wide, gain):
    inv_rms = lax.rsqrt(jnp.mean(wide * wide, axis=-1, keepdims=True) + NORM_EPS)
    return (wide * inv_rms * gain).astype(BF)


RELAY = 256
PER_REQ = OLD // RELAY
N_RELAY = REQ * PER_REQ
RSLOTS = 4
THIRDS = (0, N_RELAY // 3, 2 * N_RELAY // 3, N_RELAY)
KB = 512
FT = 256
N_FULL = FFN // FT
TAIL = FFN - N_FULL * FT
OT = 512
N_OUT = DIM // OT
NT = (((1,), (1,)), ((), ()))
TN = (((0,), (0,)), ((), ()))
SCALE = (HD ** -0.5) * 1.4426950408889634


def layer_kernel(pre_ref, val_ref, x_ref, ga_ref, gm_ref, bq_ref, bk_ref, bv_ref, kc_ref, vc_ref,
                 wq_hbm, wk_hbm, wv_hbm, wo_hbm, wg_hbm, wu_hbm, wd_hbm,
                 out_ref, kn_out, vn_out, kh_out, vh_out,
                 hbuf, part, prx, near, far, mid,
                 wsem, osem, msem, isem, csem, ksem, nsem,
                 a1send, a1recv, a2send, a2recv, psend, precv, send, nrecv, frecv):
    pos = Place()

    def span(u):
        return u // PARTS, pl.ds((u % PARTS) * UROWS, UROWS)

    def gather(u, sends, recvs):
        r, rows = span(u)
        return Gather(pos, lambda t: hbuf.at[r, t, rows], lambda n: sends.at[u, n], lambda t: recvs.at[u, t])

    def scatter(k, u):
        r, rows = span(u)
        return Scatter(
            pos, lambda t: part.at[r, t, rows], lambda dm: prx.at[r, dm, rows],
            lambda n: near.at[r, n, rows], lambda n: far.at[r, n, rows],
            lambda dm: psend.at[k, u, dm], lambda dm: precv.at[k, u, dm], lambda dm: send.at[k, u, dm],
            lambda n: nrecv.at[k, u, n], lambda n: frecv.at[k, u, n])

    g1 = [gather(u, a1send, a1recv) for u in range(UNITS)]
    g2 = [gather(u, a2send, a2recv) for u in range(UNITS)]
    rs = [[scatter(k, u) for u in range(UNITS)] for k in range(2)]

    mem = {}

    def qkv_load(n):
        return pltpu.make_async_copy((wq_hbm, wk_hbm, wv_hbm)[n], mem["wbuf"].at[n], wsem.at[n])

    def wo_load():
        return pltpu.make_async_copy(wo_hbm, mem["wo"], osem)

    def mlp_load(w):
        return pltpu.make_async_copy((wg_hbm, wu_hbm, wd_hbm)[w], mem[("wg", "wu", "wd")[w]], msem.at[w])

    def relay_in(n, w):
        rows = pl.ds(pl.multiple_of((n % PER_REQ) * RELAY * HEADS, RELAY * HEADS), RELAY * HEADS)
        slot = n % RSLOTS
        return pltpu.make_async_copy((kc_ref, vc_ref)[w].at[n // PER_REQ, rows], mem["cin"].at[slot, w], isem.at[slot, w])

    def relay_out(n, w):
        rows = pl.ds(pl.multiple_of((n % PER_REQ) * RELAY, RELAY), RELAY)
        slot = n % RSLOTS
        return pltpu.make_async_copy(mem["cout"].at[slot, w], (kh_out, vh_out)[w].at[n // PER_REQ, :, rows], csem.at[slot, w])

    def head_load(r, h, slot):
        return [pltpu.make_async_copy(src.at[r, h], mem["kv"].at[slot, w], ksem.at[slot, w])
                for w, src in enumerate((kh_out, vh_out))]

    def new_rows(r, w):
        return pltpu.make_async_copy(mem["nbuf"].at[w], (kn_out, vn_out)[w].at[r], nsem.at[w])

    def norm_rows(r):
        gain = ga_ref[...].astype(F32).reshape(1, DIM)

        def run(i, carry):
            rows = pl.ds(pl.multiple_of(i * 16, 16), 16)
            hbuf[r, pos.me, rows, :] = norm_value(x_ref[r, rows, :].astype(F32), gain)
            return carry

        lax.fori_loop(0, ROWS // 16, run, 0)

    def pre():
        for n in range(3):
            qkv_load(n).start()
        for n in range(RSLOTS - 1):
            for w in range(2):
                relay_in(n, w).start()
        norm_rows(0)
        entry_barrier(pos)

    def pre2():
        wo_load().start()
        norm_rows(1)

    def tables():
        cosb, sinb = mem["cosb"], mem["sinb"]
        half = HD // 2
        lane = lax.broadcasted_iota(jnp.int32, (1, HD), 1)
        freq_id = (lane % half).astype(F32)
        inv_freq = jnp.exp((freq_id * 2.0 / HD) * (-jnp.log(jnp.float32(ROPE_THETA))))
        sign = jnp.where(lane < half, -1.0, 1.0).astype(F32)

        def run(i, carry):
            row_pos = lax.broadcasted_iota(jnp.int32, (ROWS, 1), 0) + i * ROWS
            for r in range(REQ):
                angles = (row_pos + pre_ref[r]).astype(F32) * inv_freq
                cosb[r, i] = jnp.cos(angles)
                sinb[r, i] = jnp.sin(angles) * sign
            return carry

        lax.fori_loop(0, RANKS, run, 0)

    def relay(third):
        cin, cout, wide = mem["cin"], mem["cout"], mem["wide"]

        def run(n, carry):
            slot = n % RSLOTS
            for w in range(2):
                @pl.when(n + RSLOTS - 1 < N_RELAY)
                def _():
                    relay_in(n + RSLOTS - 1, w).start()

                relay_in(n, w).wait()

                @pl.when(n >= RSLOTS)
                def _():
                    relay_out(n - RSLOTS, w).wait()

                base = w * RELAY * HEADS
                wide[pl.ds(base, RELAY * HEADS), :] = cin[slot, w].astype(F32)
                for h in range(HEADS):
                    cout[slot, w, h] = wide[pl.ds(base + h, RELAY, stride=HEADS), :].astype(BF)
                relay_out(n, w).start()
            return carry

        lax.fori_loop(THIRDS[third], THIRDS[third + 1], run, 0)
        if third == 2:
            for n in range(N_RELAY - RSLOTS, N_RELAY):
                for w in range(2):
                    relay_out(n, w).wait()
            for cp in head_load(0, 0, 0):
                cp.start()

    def qkv(u, i):
        wbuf, qbuf, cosb, sinb, wide, nbuf = (mem[k] for k in ("wbuf", "qbuf", "cosb", "sinb", "wide", "nbuf"))
        r, rows = span(u)
        if u == 0:
            qkv_load(i).wait()
        bias = (bq_ref, bk_ref, bv_ref)[i]

        def run(tile, carry):
            cols = pl.ds(pl.multiple_of(tile * 256, 256), 256)
            lhs = hbuf[r, :, rows, :].reshape(ULEN, DIM)
            acc = jnp.dot(lhs, wbuf[i, :, cols], preferred_element_type=F32)
            val = (acc + bias[cols].astype(F32).reshape(1, 256)).astype(BF)
            for k in range(2):
                head = val[:, k * HD:(k + 1) * HD]
                if i < 2:
                    wide_head = head.astype(F32)
                    cos_t = cosb[r, :, rows, :].reshape(ULEN, HD)
                    sin_t = sinb[r, :, rows, :].reshape(ULEN, HD)
                    head = (wide_head * cos_t + pltpu.roll(wide_head, HD // 2, 1) * sin_t).astype(BF)
                qbuf[i, tile * 2 + k, :, rows, :] = head.reshape(RANKS, UROWS, HD)
            return carry

        lax.fori_loop(0, 2, run, 0)
        if i > 0 and u % PARTS == PARTS - 1:
            w = i - 1
            if r > 0:
                new_rows(r - 1, w).wait()
            for h in range(HEADS):
                wide[pl.ds(h, CHUNK, stride=HEADS), :] = qbuf[i, h].reshape(CHUNK, HD).astype(F32)
            nbuf[w] = wide[...].astype(BF)
            new_rows(r, w).start()

    def attend(r, pair):
        qbuf, obuf, kv = mem["qbuf"], mem["obuf"], mem["kv"]
        prefix = pre_ref[r]
        last = val_ref[r] - 1
        key = lax.broadcasted_iota(jnp.int32, (KB, CHUNK), 0)
        row = lax.broadcasted_iota(jnp.int32, (KB, CHUNK), 1)

        def head(h, carry):
            slot = h % 2
            for cp in head_load(r, h, slot):
                cp.wait()
            if r + 1 < REQ:
                nxt = h + 1
                more = head_load(r + nxt // HEADS, nxt % HEADS, 1 - slot)
                for cp in more:
                    cp.start()
            else:
                @pl.when(h + 1 < HEADS)
                def _():
                    for cp in head_load(r, h + 1, 1 - slot):
                        cp.start()

            q = qbuf[0, h].reshape(CHUNK, HD)

            def scores(keys):
                return lax.dot_general(keys, q, NT, preferred_element_type=F32) * SCALE

            s = jnp.where(key <= jnp.minimum(row, last), scores(qbuf[1, h].reshape(CHUNK, HD)), -1.0e30)
            m = jnp.max(s, axis=0, keepdims=True)
            probs = jnp.exp2(s - m)
            l = jnp.sum(probs, axis=0, keepdims=True)
            acc = lax.dot_general(qbuf[2, h].reshape(CHUNK, HD), probs.astype(BF), TN, preferred_element_type=F32)

            def fold(b, state):
                m, l, acc = state
                rows = pl.ds(pl.multiple_of(b * KB, KB), KB)
                s = jnp.where(key < prefix - b * KB, scores(kv[slot, 0, rows, :]), -1.0e30)
                m_new = jnp.maximum(m, jnp.max(s, axis=0, keepdims=True))
                shrink = jnp.exp2(m - m_new)
                probs = jnp.exp2(s - m_new)
                l = l * shrink + jnp.sum(probs, axis=0, keepdims=True)
                acc = acc * shrink + lax.dot_general(kv[slot, 1, rows, :], probs.astype(BF), TN, preferred_element_type=F32)
                return m_new, l, acc

            m, l, acc = lax.fori_loop(0, OLD // KB, fold, (m, l, acc))
            mixed = (acc / l).T.astype(BF).reshape(RANKS, ROWS, HD)
            obuf[r, :, :, pl.ds(pl.multiple_of(h * HD, HD), HD)] = mixed
            return carry

        lax.fori_loop(2 * pair, 2 * pair + 2, head, 0)

    def store_part(u, cols, value):
        r, rows = span(u)
        part[r, :, rows, cols] = value.astype(BF).reshape(RANKS, UROWS, OT)

    def out_proj(u):
        r, rows = span(u)
        if u % PARTS == 0:
            for part_id in range(PARTS):
                g1[u + part_id].drain()
        if u == 0:
            wo_load().wait()
        obuf, wo = mem["obuf"], mem["wo"]

        def run(n, carry):
            cols = pl.ds(pl.multiple_of(n * OT, OT), OT)
            lhs = obuf[r, :, rows, :].reshape(ULEN, QKV)
            store_part(u, cols, jnp.dot(lhs, wo[:, cols], preferred_element_type=F32))
            return carry

        lax.fori_loop(0, N_OUT, run, 0)

    def act(u, tile, size):
        r, rows = span(u)
        h = hbuf[r, :, rows, :].reshape(ULEN, DIM)
        gate = lax.dot_general(h, mem["wg"][tile, :], NT, preferred_element_type=F32)
        up = lax.dot_general(h, mem["wu"][tile, :], NT, preferred_element_type=F32)
        mem["ubuf"][:, tile] = (gate * (1.0 / (1.0 + jnp.exp(-gate))) * up).astype(BF)

    def mlp_up(u, k):
        if u == 0 and k == 0:
            mlp_load(0).wait()
            mlp_load(1).wait()

        def run(n, carry):
            act(u, pl.ds(pl.multiple_of(n * FT, FT), FT), FT)
            return carry

        if k < 2:
            lax.fori_loop(2 * k, (2, N_FULL)[k], run, 0)
        else:
            act(u, slice(N_FULL * FT, FFN), TAIL)

    def mlp_down(u, k):
        if k == 0:
            rs[0][u].drain()
        if u == 0 and k == 0:
            mlp_load(2).wait()

        def run(n, carry):
            cols = pl.ds(pl.multiple_of(n * OT, OT), OT)
            store_part(u, cols, jnp.dot(mem["ubuf"][...], mem["wd"][:, cols], preferred_element_type=F32))
            return carry

        lax.fori_loop(k * N_OUT // 2, (k + 1) * N_OUT // 2, run, 0)

    def summed(refs, rows):
        total = refs[0][rows, :].astype(F32)
        for ref in refs[1:]:
            total = total + ref[rows, :].astype(F32)
        return total.astype(BF).astype(F32)

    def mid_rows(u):
        def use(refs):
            gain = gm_ref[...].astype(F32).reshape(1, DIM)
            r = u // PARTS

            def body(row):
                own = pl.ds(row + (u % PARTS) * UROWS, 16)
                x1 = (x_ref[r, own, :].astype(F32) + summed(refs, pl.ds(row, 16))).astype(BF)
                mid[r, own, :] = x1
                hbuf[r, pos.me, own, :] = norm_value(x1.astype(F32), gain)

            row_loop(body)

        return use

    def out_rows(u):
        def use(refs):
            r = u // PARTS

            def body(row):
                own = pl.ds(row + (u % PARTS) * UROWS, 16)
                out_ref[r, own, :] = (mid[r, own, :].astype(F32) + summed(refs, pl.ds(row, 16))).astype(BF)

            row_loop(body)

        return use

    local = {"pre": pre, "pre2": pre2, "rl": relay, "cs": tables, "qkv": qkv, "at": attend,
             "wo": out_proj, "up": mlp_up, "dn": mlp_down}
    remote = {
        "a1": lambda u, i, q: g1[u].step(i, q),
        "a2": lambda u, i, q: g2[u].step(i, q),
        "sw1": lambda u, q: rs[0][u].swap(),
        "sw2": lambda u, q: rs[1][u].swap(),
        "st1": lambda u, i, q: rs[0][u].step(i, q),
        "st2": lambda u, i, q: rs[1][u].step(i, q),
        "fi1": lambda u, q: rs[0][u].final(q, mid_rows(u)),
        "fi2": lambda u, q: rs[1][u].final(q, out_rows(u)),
    }
    pending = []

    def flush():
        for q in (0, 1):
            mine = [op for op in pending if op[-1] == q]
            if mine:
                def run():
                    for op in mine:
                        remote[op[0]](*op[1:])

                pos.role(q, run)
        pending.clear()

    def play(ops):
        for op in ops:
            if op[0] in remote:
                pending.append(op)
            else:
                flush()
                local[op[0]](*op[1:])
        flush()

    cut = ORDER.index(("wo", UNITS - 1)) + 1

    def attention_phase(**refs):
        mem.update(refs)
        play(ORDER[:cut])
        for w in range(2):
            new_rows(REQ - 1, w).wait()

    def mlp_phase(**refs):
        mem.update(refs)
        for w in range(3):
            mlp_load(w).start()
        play(ORDER[cut:])

    pl.run_scoped(
        attention_phase,
        wbuf=pltpu.VMEM((3, DIM, QKV), BF),
        wo=pltpu.VMEM((QKV, DIM), BF),
        kv=pltpu.VMEM((2, 2, OLD, HD), BF),
        qbuf=pltpu.VMEM((3, HEADS, RANKS, ROWS, HD), BF),
        obuf=pltpu.VMEM((REQ, RANKS, ROWS, QKV), BF),
        cosb=pltpu.VMEM((REQ, RANKS, ROWS, HD), F32),
        sinb=pltpu.VMEM((REQ, RANKS, ROWS, HD), F32),
        cin=pltpu.VMEM((RSLOTS, 2, RELAY * HEADS, HD), BF),
        cout=pltpu.VMEM((RSLOTS, 2, HEADS, RELAY, HD), BF),
        wide=pltpu.VMEM((2 * RELAY * HEADS, HD), F32),
        nbuf=pltpu.VMEM((2, CHUNK * HEADS, HD), BF),
    )
    pl.run_scoped(
        mlp_phase,
        wg=pltpu.VMEM((FFN, DIM), BF),
        wu=pltpu.VMEM((FFN, DIM), BF),
        wd=pltpu.VMEM((FFN, DIM), BF),
        ubuf=pltpu.VMEM((ULEN, FFN), BF),
    )
    for u in range(UNITS):
        g2[u].drain()
        rs[1][u].drain()


def run_layer(prefix, valid, x_rows, g_attn, g_mlp, b_q, b_k, b_v, k_flat, v_flat, w_q, w_k, w_v, w_o, w_gate_t, w_up_t, w_down):
    vm = pl.BlockSpec(memory_space=pltpu.VMEM)
    sm = pl.BlockSpec(memory_space=pltpu.SMEM)
    anyspace = pl.BlockSpec(memory_space=pl.ANY)
    dma = pltpu.SemaphoreType.DMA
    fresh = jax.ShapeDtypeStruct((REQ, CHUNK * HEADS, HD), BF)
    old = jax.ShapeDtypeStruct((REQ, HEADS, OLD, HD), BF)
    block = (ROWS, DIM)
    return pl.pallas_call(
        layer_kernel,
        out_shape=(jax.ShapeDtypeStruct((REQ,) + block, BF), fresh, fresh, old, old),
        in_specs=[sm, sm] + [vm] * 6 + [anyspace] * 9,
        out_specs=[vm] + [anyspace] * 4,
        scratch_shapes=[
            pltpu.VMEM((REQ, RANKS) + block, BF),
            pltpu.VMEM((REQ, RANKS) + block, BF),
            pltpu.VMEM((REQ, 4) + block, BF),
            pltpu.VMEM((REQ, 3) + block, BF),
            pltpu.VMEM((REQ, 2) + block, BF),
            pltpu.VMEM((REQ,) + block, BF),
            dma((3,)), dma, dma((3,)), dma((RSLOTS, 2)), dma((RSLOTS, 2)), dma((2, 2)), dma((2,)),
            dma((UNITS, 9)), dma((UNITS, RANKS)), dma((UNITS, 9)), dma((UNITS, RANKS)),
            dma((2, UNITS, 4)), dma((2, UNITS, 4)), dma((2, UNITS, 4)), dma((2, UNITS, 3)), dma((2, UNITS, 2)),
        ],
        compiler_params=pltpu.CompilerParams(collective_id=0, has_side_effects=True, vmem_limit_bytes=67043328),
        name="layer",
    )(prefix, valid, x_rows, g_attn, g_mlp, b_q, b_k, b_v, k_flat, v_flat, w_q, w_k, w_v, w_o, w_gate_t, w_up_t, w_down)


COPY = 1024
N_COPY = SLOTS // COPY


def cache_kernel(pre_ref, val_ref, kc_hbm, vc_hbm, krow_hbm, vrow_hbm, kout_hbm, vout_hbm,
                 cbuf, nbuf, isem, osem, nsem, usem):
    srcs = (kc_hbm, vc_hbm)
    dsts = (kout_hbm, vout_hbm)
    news = (krow_hbm, vrow_hbm)
    groups = [(w, i) for w in range(2) for i in range(REQ)]

    def takes(w, i):
        return [pltpu.make_async_copy(srcs[w].at[i, pl.ds(n * COPY, COPY)], cbuf.at[w, i, pl.ds(n * COPY, COPY)], isem.at[w, i, n])
                for n in range(N_COPY)]

    def puts(w, i):
        return [pltpu.make_async_copy(cbuf.at[w, i, pl.ds(n * COPY, COPY)], dsts[w].at[i, pl.ds(n * COPY, COPY)], osem.at[w, i, n])
                for n in range(N_COPY)]

    def updates(w, i, act):
        count = val_ref[i]
        for bit in range(10):
            size = 1 << bit
            first = (count >> (bit + 1)) << (bit + 1)

            @pl.when((count >> bit) % 2 == 1)
            def _():
                act(pltpu.make_async_copy(
                    nbuf.at[w, i, pl.ds(first, size)],
                    cbuf.at[w, i, pl.ds(pre_ref[i] + first, size)],
                    usem.at[w, i, bit]))

    fresh = [pltpu.make_async_copy(news[w], nbuf.at[w], nsem.at[w]) for w in range(2)]
    for w, i in groups:
        for cp in takes(w, i):
            cp.start()
        if i == 0:
            fresh[w].start()
    for w, i in groups:
        for cp in takes(w, i):
            cp.wait()
        if i == 0:
            fresh[w].wait()
        updates(w, i, lambda cp: cp.start())
        updates(w, i, lambda cp: cp.wait())
        for cp in puts(w, i):
            cp.start()
    for w, i in groups:
        for cp in puts(w, i):
            cp.wait()


def run_cache(prefix, valid, k_cache, v_cache, k_rows, v_rows):
    sm = pl.BlockSpec(memory_space=pltpu.SMEM)
    anyspace = pl.BlockSpec(memory_space=pl.ANY)
    dma = pltpu.SemaphoreType.DMA
    cache = jax.ShapeDtypeStruct((REQ, SLOTS, HEADS, HD), BF)
    return pl.pallas_call(
        cache_kernel,
        out_shape=(cache, cache),
        in_specs=[sm, sm] + [anyspace] * 4,
        out_specs=[anyspace] * 2,
        scratch_shapes=[
            pltpu.VMEM((2, REQ, SLOTS, HEADS, HD), BF),
            pltpu.VMEM((2, REQ, CHUNK, HEADS, HD), BF),
            dma((2, REQ, N_COPY)), dma((2, REQ, N_COPY)), dma((2,)), dma((2, REQ, 10)),
        ],
        compiler_params=pltpu.CompilerParams(vmem_limit_bytes=60 << 20),
        name="cache_write",
    )(prefix, valid, k_cache, v_cache, k_rows, v_rows)


def solution(mesh):
    row_spec = P("dp", "tp", None)
    cache_spec = P("dp", None, "tp", None)
    req_spec = P("dp")
    rep_spec = P(None)
    col_spec = P(None, "tp")
    bias_spec = P("tp")
    down_spec = P("tp", None)

    def layer(x_rows, k_cache, v_cache, prefix, valid, g_attn, w_q, b_q, w_k, b_k, w_v, b_v, w_o, g_mlp, w_gate, w_up, w_down):
        flat = (REQ, SLOTS * HEADS, HD)
        wide = (REQ, CHUNK, HEADS, HD)
        x_out, k_rows, v_rows, _, _ = run_layer(
            prefix, valid, x_rows, g_attn, g_mlp, b_q, b_k, b_v, k_cache.reshape(flat), v_cache.reshape(flat),
            w_q, w_k, w_v, w_o, w_gate.T, w_up.T, w_down)
        k_out, v_out = run_cache(prefix, valid, k_cache, v_cache, k_rows.reshape(wide), v_rows.reshape(wide))
        return x_out, k_out, v_out

    in_specs = (row_spec, cache_spec, cache_spec, req_spec, req_spec, rep_spec, col_spec, bias_spec, col_spec, bias_spec, col_spec, bias_spec, down_spec, rep_spec, col_spec, col_spec, down_spec)
    return jax.shard_map(layer, mesh=mesh, in_specs=in_specs, out_specs=(row_spec, cache_spec, cache_spec), check_vma=False)
```
